32 devices in a mesh: slab: 8 (over z, x), row: 4 (over y, core).
Axes of the slice: x: 2, y: 2, z: 4, core: 2. Of those that a mesh axis runs over, the one named last changes fastest.
Arguments:
- slot_brick: int32 [32, 32, 2], P(('slab', 'row')), may hold values from 0 to 255
- slot_count: int32 [32, 32, 2], P(('slab', 'row')), may hold values from 1 to 64, as said below
- point_cell: int32 [32, 32, 2, 64], P(('slab', 'row')), may hold values from 0 to 1023
- point_frac: float32 [32, 32, 2, 64], P(('slab', 'row')), may hold values from -0.5 to 0.5
- point_normal: float32 [32, 32, 2, 3, 64], P(('slab', 'row')), may hold values from -6 to 6
- point_weight: float32 [32, 32, 2, 64], P(('slab', 'row')), may hold values from 0.2 to 2
- guess: float32 [128, 64, 1024], P('slab', 'row'), may hold values from -4 to 4
Outputs:
- indicator: float32 [128, 64, 1024], P('slab', 'row')
The draws below stay inside these ranges and needn't reach their ends.
Inputs may be any that keep to these rules, and one draw needn't show every extreme that they name: `slot_count`: every source block has at least one slot with exactly 64 live points.
All inputs are finite; a program needn't handle non-finite values.
Results may differ from the reference program's by a relative error of at most 0.0003.
Values sent between devices are 32-bit elements; how exact they have to be, the bound alone decides.
No kernel may reach another device: no remote copies, remote signals or barrier semaphores. Data moves between devices by JAX's collectives and lax.ppermute only.
A program may use at most 64 MiB of HBM per device.

```python
import math
import jax
import jax.numpy as jnp
from jax import lax

Z_DEV = 16
Y_DEV = 16
NX = 1024
CAP = 64
S_PEER = 2
SWEEPS = 3
NZ = 128
NY = 64
BRICKS_DEV = 256
N_ROW = 4
DEVICES = 32


def draw_slot_count(key, part):
    first, second = jax.random.split(jax.random.fold_in(key, 17))
    base = jax.random.randint(first, (DEVICES, DEVICES * S_PEER), 1, CAP + 1)
    chosen = jax.random.randint(second, (DEVICES,), 0, DEVICES * S_PEER)
    lanes = jnp.arange(DEVICES * S_PEER, dtype=jnp.int32)
    filled = jnp.where(lanes[None, :] == chosen[:, None], CAP, base)
    return filled.reshape(DEVICES, DEVICES, S_PEER).astype(jnp.int32)


def touch_ends(values, stream_key, low, top_value):
    spot = [jax.random.randint(jax.random.fold_in(stream_key, axis), (), 0, length) for axis, length in enumerate(values.shape)]
    main_axis = values.shape.index(max(values.shape))
    neighbour = spot[:main_axis] + [(spot[main_axis] + 1) % values.shape[main_axis]] + spot[main_axis + 1:]
    return values.at[tuple(spot)].set(low).at[tuple(neighbour)].set(top_value)


def steps_of(stream_key, dims, shards, least, top_value):
    def one(axis_at, blocks):
        steps = jax.random.uniform(jax.random.fold_in(jax.random.fold_in(stream_key, 6), axis_at), (blocks,), jnp.float32, least / len(shards), top_value / len(shards))
        return jnp.repeat(jnp.exp(steps), dims[axis_at] // blocks).reshape((-1,) + (1,) * (len(dims) - axis_at - 1))

    loudness = one(*shards[0])
    for cut in shards[1:]:
        loudness = loudness * one(*cut)
    return loudness


def bell_draw(rng, shape, width, bound, shards=(), kind=jnp.bfloat16):
    drawn = jax.random.normal(rng, shape, jnp.float32) * width
    if len(shards) > 0:
        drawn = steps_of(rng, shape, shards, -0.22, 0.18) * drawn
    return jnp.clip(drawn, min=-bound, max=bound).astype(kind)


def setup_inputs(seed: int = 0) -> dict:
    keys = jax.random.split(jax.random.key(seed), 8)
    slot_brick = touch_ends(jax.random.randint(keys[0], (DEVICES, DEVICES, S_PEER), 0, BRICKS_DEV), jax.random.fold_in(keys[0], 1), 0, BRICKS_DEV - 1).astype(jnp.int32)
    slot_count = draw_slot_count(jax.random.fold_in(keys[7], 71), 0)
    point_cell = touch_ends(jax.random.randint(keys[2], (DEVICES, DEVICES, S_PEER, CAP), 0, NX), jax.random.fold_in(keys[2], 1), 0, NX - 1).astype(jnp.int32)
    point_frac = jnp.clip(jax.random.uniform(keys[3], (DEVICES, DEVICES, S_PEER, CAP), jnp.float32, -0.5, 0.5) * steps_of(keys[3], (DEVICES, DEVICES, S_PEER, CAP), ((0, 32),), -0.4, 0.0), -0.5, 0.5)
    point_normal = bell_draw(keys[4], (DEVICES, DEVICES, S_PEER, 3, CAP), 1.0, 6.0, ((0, 32),), jnp.float32)
    point_weight = jnp.clip(jnp.exp(math.log(2.0) - 2.3025851 * jax.random.uniform(keys[5], (DEVICES, DEVICES, S_PEER, CAP), jnp.float32) ** steps_of(keys[5], (DEVICES, DEVICES, S_PEER, CAP), ((0, 32),), -0.2, 0.2)), 0.2, 2.0)
    guess = bell_draw(keys[6], (NZ, NY, NX), 0.5, 4.0, ((0, 8), (1, 4)), jnp.float32)
    return dict(slot_brick=slot_brick, slot_count=slot_count, point_cell=point_cell, point_frac=point_frac, point_normal=point_normal, point_weight=point_weight, guess=guess)


HIGH = lax.Precision.HIGHEST
ALPHA = 4.0


def splat_block(cell, frac, count, values):
    lanes = jnp.arange(cell.shape[1], dtype=jnp.int32)
    live = (lanes[None, :] < count[:, None]).astype(jnp.float32)
    low = 0.5 * (0.5 - frac) ** 2 * live
    middle = (0.75 - frac * frac) * live
    high = 0.5 * (0.5 + frac) ** 2 * live
    cells = jnp.arange(NX, dtype=jnp.int32)
    delta = cells[None, None, :] - cell[:, :, None]
    table = jnp.where(delta == -1, low[..., None], jnp.where(delta == 0, middle[..., None], jnp.where(delta == 1, high[..., None], jnp.float32(0.0))))
    return jnp.einsum("nkp,npx->nkx", values, table, precision=HIGH)


def along(array, axis, kind):
    size = array.shape[axis] - 2
    lower = lax.slice_in_dim(array, 0, size, axis=axis)
    centre = lax.slice_in_dim(array, 1, size + 1, axis=axis)
    upper = lax.slice_in_dim(array, 2, size + 2, axis=axis)
    if kind == "mass":
        return (lower + 4.0 * centre + upper) / 6.0
    return 2.0 * centre - lower - upper


def stiffness(padded):
    mass_x = along(padded, 2, "mass")
    stiff_x = along(padded, 2, "stiff")
    return (along(along(mass_x, 1, "mass"), 0, "stiff") + along(along(mass_x, 1, "stiff"), 0, "mass")
            + along(along(stiff_x, 1, "mass"), 0, "mass"))


def reference(slot_brick, slot_count, point_cell, point_frac, point_normal, point_weight, guess):
    total = DEVICES * DEVICES * S_PEER
    block = 64
    dest = jnp.broadcast_to(jnp.arange(DEVICES, dtype=jnp.int32)[None, :, None], slot_brick.shape)
    global_z = (dest // N_ROW) * Z_DEV + slot_brick // Y_DEV
    global_y = (dest % N_ROW) * Y_DEV + slot_brick % Y_DEV
    target = (global_z * NY + global_y).reshape(total // block, block)
    cells = point_cell.reshape(total // block, block, CAP)
    fracs = point_frac.reshape(total // block, block, CAP)
    counts = slot_count.reshape(total // block, block)
    values = jnp.concatenate([point_normal, point_weight[:, :, :, None, :]], axis=3).reshape(total // block, block, 4, CAP)

    def step(field, item):
        where, cell, frac, count, value = item
        return field.at[where].add(splat_block(cell, frac, count, value)), None

    start = jnp.zeros((NZ * NY, 4, NX), jnp.float32)
    field, _ = lax.scan(step, start, (target, cells, fracs, counts, values))
    field = jnp.transpose(field.reshape(NZ, NY, 4, NX), (2, 0, 1, 3))
    padded = jnp.pad(field[0:3], ((0, 0), (1, 1), (1, 1), (1, 1)))
    spread = (padded[0, 1:-1, 1:-1, 2:] - padded[0, 1:-1, 1:-1, :-2]
              + padded[1, 1:-1, 2:, 1:-1] - padded[1, 1:-1, :-2, 1:-1]
              + padded[2, 2:, 1:-1, 1:-1] - padded[2, :-2, 1:-1, 1:-1])
    rhs = -0.5 * spread
    density = field[3]
    inverse = 1.0 / (8.0 / 3.0 + ALPHA * density)
    parity = (jnp.arange(NZ, dtype=jnp.int32)[:, None, None] + jnp.arange(NY, dtype=jnp.int32)[None, :, None]
              + jnp.arange(NX, dtype=jnp.int32)[None, None, :]) % 2
    indicator = guess
    for sweep in range(SWEEPS):
        for colour in (0, 1):
            mask = (parity == colour).astype(jnp.float32)
            residue = rhs - stiffness(jnp.pad(indicator, 1)) - ALPHA * density * indicator
            indicator = indicator + mask * residue * inverse
    return indicator
```

```python
import functools
import jax
import jax.numpy as jnp
from jax import lax
from jax.experimental import pallas as pl
from jax.experimental.pallas import tpu as pltpu
from jax.sharding import PartitionSpec as P

Z_DEV = 16
Y_DEV = 16
NX = 1024
CAP = 64
S_PEER = 2
SWEEPS = 3
ALPHA = 4.0

HALO = 2 * SWEEPS
EXT = Z_DEV + 2 * HALO
PAIRS = EXT // 2
RIM = EXT + 2
LANES = 128
SUB = NX // LANES
CODE = 16384
UNROLL = 8
F32 = jnp.float32
BF16 = jnp.bfloat16


def chain(axis, step):
    size = lax.axis_size(axis)
    return [(i, i + step) for i in range(size) if 0 <= i + step < size]


def relax_kernel(tiles, codes, flags, guess, zlo, zhi, pay_own, pay_lo, pay_hi, out,
                 prep, acc, vr, vb, gr, gb, ir, ib, sx, st, qa, todo):
    slots = tiles * S_PEER
    halo_rows = EXT * HALO * SUB
    lane = lax.broadcasted_iota(jnp.int32, (SUB, LANES), 1)
    sub = lax.broadcasted_iota(jnp.int32, (SUB, LANES), 0)
    low = lane < CAP
    even = lane % 2 == 0
    first_lane = lane == 0
    last_lane = lane == LANES - 1
    keep_up = (sub > 0).astype(F32)
    keep_dn = (sub < SUB - 1).astype(F32)
    zero = jnp.zeros((SUB, LANES), F32)

    def parity(p):
        return even if p % 2 == 0 else jnp.logical_not(even)

    def shifts(v):
        up = jnp.where(last_lane, pltpu.roll(v, 1, 0) * keep_up, v)
        dn = jnp.where(first_lane, pltpu.roll(v, SUB - 1, 0) * keep_dn, v)
        return pltpu.roll(up, 1, 1), pltpu.roll(dn, LANES - 1, 1)

    def scan(i, pos):
        for u in range(8):
            e = codes[i * 8 + u]
            todo[pos] = e
            pos = pos + (e >= 0).astype(jnp.int32)
        return pos

    count = lax.fori_loop(0, 3 * slots // 8, scan, jnp.int32(0))
    dummy = (RIM + 1) * CODE + 3 * slots
    for u in range(UNROLL):
        todo[count + u] = jnp.int32(dummy)

    def clear(i, _):
        for u in range(12):
            acc[i * 12 + u] = zero
        return 0

    lax.fori_loop(0, 3 * RIM * RIM // 12, clear, 0)

    for block, (pay, base) in enumerate(((pay_own, 0), (pay_lo, halo_rows), (pay_hi, halo_rows))):
        def prepare(i, _, pay=pay, base=base, block=block):
            for s in range(S_PEER):
                rows = [pay[pl.ds(base + i * 64 + 2 * r + s, 8, stride=8), :] for r in range(3)]
                turned = [pltpu.roll(x, CAP, 1) for x in rows]
                cell = jnp.where(low, rows[0], turned[0])
                frac = jnp.where(low, turned[0], rows[0])
                vals = []
                for r in (1, 2):
                    vals.append(jnp.where(low, rows[r], turned[r]))
                    vals.append(jnp.where(low, turned[r], rows[r]))
                less = 0.5 - frac
                more = 0.5 + frac
                weights = (
                    jnp.where(low, 0.5 * less * less, 0.75 - frac * frac),
                    jnp.where(low, 0.5 * more * more, 0.0),
                )
                whole = cell.astype(jnp.int32)
                at = pl.multiple_of(block * slots + (i * 2 + s) * 8, 8)
                for h in range(2):
                    c = jnp.where(low, whole - 1, whole) if h == 0 else whole + 1
                    prep[16 + h, pl.ds(at, 8), :] = (c >> 7).astype(F32)
                    prep[18 + h, pl.ds(at, 8), :] = (c & 127).astype(F32)
                    for ch in range(4):
                        v = vals[ch] * weights[h]
                        head = v.astype(BF16).astype(F32)
                        prep[h * 8 + ch, pl.ds(at, 8), :] = head
                        prep[h * 8 + 4 + ch, pl.ds(at, 8), :] = v - head
            return 0

        lax.fori_loop(0, tiles // 8, prepare, 0)
    for q in range(20):
        prep[q, pl.ds(3 * slots, 8), :] = zero

    subf = sub.astype(F32)
    col = lax.broadcasted_iota(jnp.int32, (LANES, LANES), 0).astype(F32).astype(BF16)
    one = jnp.ones((LANES, LANES), BF16)
    nil = jnp.zeros((LANES, LANES), BF16)

    def splat(i, _):
        for u in range(UNROLL):
            e = todo[i * UNROLL + u]
            centre = e // CODE
            row = e % CODE
            lhs, rhs = [], []
            for h in range(2):
                hi = jnp.broadcast_to(prep[16 + h, pl.ds(row, 1), :], (SUB, LANES))
                hit = hi == subf
                parts = [
                    jnp.where(hit, jnp.broadcast_to(prep[h * 8 + q, pl.ds(row, 1), :], (SUB, LANES)), 0.0)
                    for q in range(8)
                ]
                lhs.append(jnp.concatenate(parts, axis=0))
                lo = jnp.broadcast_to(prep[18 + h, pl.ds(row, 1), :], (LANES, LANES)).astype(BF16)
                rhs.append(jnp.where(lo == col, one, nil))
            left = jnp.concatenate(lhs, axis=1).astype(BF16)
            right = jnp.concatenate(rhs, axis=1)
            res = lax.dot_general(left, right, (((1,), (1,)), ((), ())), preferred_element_type=F32)
            f = [res[ch * 8:ch * 8 + 8] + res[32 + ch * 8:40 + ch * 8] for ch in range(4)]
            size = RIM * RIM
            acc[centre] += f[0]
            acc[size + centre] += f[3]
            acc[2 * size + centre + 1] += f[1]
            acc[2 * size + centre - 1] -= f[1]
            acc[2 * size + centre + RIM] += f[2]
            acc[2 * size + centre - RIM] -= f[2]
        return 0

    lax.fori_loop(0, (count + UNROLL - 1) // UNROLL, splat, 0)

    def pack_v(z, zp, row_of):
        m = parity(zp)
        for j in range(PAIRS):
            a, b = row_of(2 * j), row_of(2 * j + 1)
            vr[z * PAIRS + j] = jnp.where(m, a, b)
            vb[z * PAIRS + j] = jnp.where(m, b, a)

    def make_rows(src, zi, z):
        def row_of(y):
            if y < HALO:
                return pay_lo[pl.ds((z * HALO + y) * SUB, SUB), :]
            if y >= HALO + Y_DEV:
                return pay_hi[pl.ds((z * HALO + y - HALO - Y_DEV) * SUB, SUB), :]
            y = y - HALO
            return src[zi, y // 8, pl.ds(y % 8, 8, stride=8), :]
        return row_of

    def pack_low(i, _):
        for u in range(2):
            pack_v(i * 2 + u, u, make_rows(zlo, i * 2 + u, i * 2 + u))
            z = HALO + Z_DEV + i * 2 + u
            pack_v(z, u, make_rows(zhi, i * 2 + u, z))
        return 0

    def pack_mid(i, _):
        for u in range(2):
            pack_v(HALO + i * 2 + u, u, make_rows(guess, i * 2 + u, HALO + i * 2 + u))
        return 0

    lax.fori_loop(0, HALO // 2, pack_low, 0)
    lax.fori_loop(0, Z_DEV // 2, pack_mid, 0)

    at_zlo, at_zhi, at_ylo, at_yhi = (flags[k] for k in range(4))

    def finish(i, _):
        for u in range(2):
            z = 1 + i * 2 + u
            m = parity(1 + u)
            fz = jnp.where(z < HALO, at_zlo, jnp.where(z >= HALO + Z_DEV, at_zhi, 1))
            size = RIM * RIM
            for j in range(PAIRS):
                fy = at_ylo if j < HALO // 2 else at_yhi if j >= (HALO + Y_DEV) // 2 else None
                f = fz if fy is None else fz * fy
                scale = jnp.broadcast_to(f.astype(F32) * (1.0 / 12.0), (SUB, LANES))
                r = (z + 1) * RIM + 2 * j + 1
                xa, xb = acc[r], acc[r + 1]
                da, db = acc[size + r], acc[size + r + 1]
                ra, rb = acc[2 * size + r], acc[2 * size + r + 1]
                xr, xbk = jnp.where(m, xa, xb), jnp.where(m, xb, xa)
                bu, bd = shifts(xbk)
                ru, rd = shifts(xr)
                gr[z * PAIRS + j] = jnp.where(m, ra, rb) + (bd - bu)
                gb[z * PAIRS + j] = jnp.where(m, rb, ra) + (rd - ru)
                ir[z * PAIRS + j] = scale / (8.0 / 3.0 + ALPHA * jnp.where(m, da, db))
                ib[z * PAIRS + j] = scale / (8.0 / 3.0 + ALPHA * jnp.where(m, db, da))
        return 0

    lax.fori_loop(0, (EXT - 2) // 2, finish, 0)

    for k in range(1, HALO + 1):
        colour = (k - 1) % 2
        vx, vy = (vr, vb) if colour == 0 else (vb, vr)
        gx, ix = (gr, ir) if colour == 0 else (gb, ib)
        j0, j1 = k // 2, PAIRS - 1 - k // 2
        wide = [j for j in range(j0 - 1, j1 + 2) if 0 <= j < PAIRS]

        def sides(p, slot, vx=vx, vy=vy, wide=wide):
            res = []
            for j in wide:
                x, y = vx[p * PAIRS + j], vy[p * PAIRS + j]
                xu, xd = shifts(x)
                yu, yd = shifts(y)
                res.append((j, xu + xd, (x + x) + (yu + yd)))
            return res

        def keep(res, slot):
            for j, s, t in res:
                sx[slot * PAIRS + j] = s
                st[slot * PAIRS + j] = t

        def advance(p, pp, slot, update, mid, colour=colour, vx=vx, gx=gx, ix=ix, j0=j0, j1=j1, wide=wide):
            m = parity(colour + pp)
            s = {j: sx[slot * PAIRS + j] for j in wide}
            t = {j: st[slot * PAIRS + j] for j in wide}
            for j in range(j0, j1 + 1):
                sl, sh = s.get(j - 1, zero), s.get(j + 1, zero)
                tl, th = t.get(j - 1, zero), t.get(j + 1, zero)
                q = (s[j] + s[j]) + t[j] + jnp.where(m, th, tl)
                if update:
                    at = (p - 1) * PAIRS + j
                    vx[at] = ix[at] * (gx[at] + (qa[PAIRS + j] + q))
                if mid:
                    d = s[j] + jnp.where(m, sl, sh)
                    qa[PAIRS + j] = (d + d) + qa[j]
                qa[j] = q

        first = k - 1
        keep(sides(first, 0), 0)
        keep(sides(first + 1, 1), 1)
        ahead = sides(first + 2, 0)
        advance(first, first, 0, False, False)
        keep(ahead, 0)
        ahead = sides(first + 3, 1)
        advance(first + 1, first + 1, 1, False, True)
        keep(ahead, 1)
        last = EXT - k

        def body(i, _, first=first, last=last):
            p = first + 2 + i * 2
            nxt0 = sides(jnp.minimum(p + 2, EXT - 1), 0)
            nxt1 = sides(jnp.minimum(p + 3, EXT - 1), 1)
            advance(p, first, 0, True, True)
            advance(p + 1, first + 1, 1, True, True)
            keep(nxt0, 0)
            keep(nxt1, 1)
            return 0

        lax.fori_loop(0, (last - first - 1) // 2, body, 0)

    def unpack(i, _):
        for u in range(2):
            z = HALO + i * 2 + u
            m = parity(u)
            for j in range(HALO // 2, (HALO + Y_DEV) // 2):
                r, b = vr[z * PAIRS + j], vb[z * PAIRS + j]
                y = 2 * j - HALO
                out[i * 2 + u, y // 8, pl.ds(y % 8, 8, stride=8), :] = jnp.where(m, r, b)
                out[i * 2 + u, y // 8, pl.ds(y % 8 + 1, 8, stride=8), :] = jnp.where(m, b, r)
        return 0

    lax.fori_loop(0, Z_DEV // 2, unpack, 0)


def as_tiles(a):
    d = a.shape[0]
    a = a.reshape(d, Y_DEV // 8, 8, SUB, LANES).transpose(0, 1, 3, 2, 4)
    return a.reshape(d, Y_DEV // 8, 8 * SUB, LANES)


def shards(slot_brick, slot_count, point_cell, point_frac, point_normal, point_weight, guess):
    n_slab, n_row = lax.axis_size("slab"), lax.axis_size("row")
    peers = point_cell.shape[1]
    tiles = 3 * peers
    slots = tiles * S_PEER

    lanes = jnp.arange(CAP, dtype=jnp.int32)
    live = (lanes < slot_count[0][:, :, None]).astype(F32)
    n = point_normal[0]
    rows0 = jnp.concatenate([point_cell[0].astype(F32), point_frac[0]], axis=-1)
    rows1 = jnp.concatenate([n[:, :, 0] * (-6.0 * live), n[:, :, 1] * (6.0 * live)], axis=-1)
    rows2 = jnp.concatenate([n[:, :, 2] * (6.0 * live), point_weight[0] * live], axis=-1)
    brick = jnp.pad((slot_brick[0] + 1).astype(F32)[:, None, :], ((0, 0), (0, 1), (0, LANES - S_PEER)))
    tile = jnp.concatenate([rows0, rows1, rows2, brick], axis=1).reshape(n_slab, n_row, 8, LANES)
    gap = jnp.zeros((1, n_row, 8, LANES), F32)
    below = jnp.concatenate([gap, tile[:-1]], axis=0)
    above = jnp.concatenate([tile[1:], gap], axis=0)
    send = jnp.stack([below, tile, above], axis=2).reshape(peers, 3, 8, LANES)

    zlo = lax.ppermute(guess[Z_DEV - HALO:], "slab", chain("slab", 1))
    zhi = lax.ppermute(guess[:HALO], "slab", chain("slab", -1))
    got = lax.all_to_all(send, ("slab", "row"), split_axis=0, concat_axis=0, tiled=True)
    points = got.reshape(tiles * 8, LANES)

    tall = jnp.concatenate([zlo, guess, zhi], axis=0)
    top = tall[:, Y_DEV - HALO:].reshape(EXT * HALO * SUB, LANES)
    bottom = tall[:, :HALO].reshape(EXT * HALO * SUB, LANES)
    pay_lo = lax.ppermute(jnp.concatenate([top, points], axis=0), "row", chain("row", 1))
    pay_hi = lax.ppermute(jnp.concatenate([bottom, points], axis=0), "row", chain("row", -1))

    halo_rows = EXT * HALO * SUB
    codes = []
    t = jnp.arange(tiles, dtype=jnp.int32)[:, None]
    s = jnp.arange(S_PEER, dtype=jnp.int32)[None, :]
    prow = ((t // 8) * 2 + s) * 8 + t % 8
    for block, (part, dy) in enumerate(((points, 0), (pay_lo[halo_rows:], -1), (pay_hi[halo_rows:], 1))):
        b = part.reshape(tiles, 8, LANES)[:, 6, :S_PEER].astype(jnp.int32) - 1
        ze = b // Y_DEV + HALO + Z_DEV * (t % 3 - 1)
        ye = b % Y_DEV + HALO + Y_DEV * dy
        inside = (b >= 0) & (ze >= 0) & (ze < EXT) & (ye >= 0) & (ye < EXT)
        entry = ((ze + 1) * RIM + ye + 1) * CODE + block * slots + prow
        codes.append(jnp.where(inside, entry, -1).reshape(-1))
    codes = jnp.concatenate(codes)
    zi, yi = lax.axis_index("slab"), lax.axis_index("row")
    flags = jnp.stack([zi > 0, zi < n_slab - 1, yi > 0, yi < n_row - 1]).astype(jnp.int32)

    vmem = pl.BlockSpec(memory_space=pltpu.VMEM)
    smem = pl.BlockSpec(memory_space=pltpu.SMEM)
    packed = pltpu.VMEM((EXT * PAIRS, SUB, LANES), F32)
    out = pl.pallas_call(
        functools.partial(relax_kernel, tiles),
        out_shape=jax.ShapeDtypeStruct((Z_DEV, Y_DEV // 8, 8 * SUB, LANES), F32),
        in_specs=[smem, smem] + [vmem] * 6,
        out_specs=vmem,
        scratch_shapes=[
            pltpu.VMEM((20, 3 * slots + 8, LANES), F32),
            pltpu.VMEM((3 * RIM * RIM, SUB, LANES), F32),
            packed, packed, packed, packed, packed, packed,
            pltpu.VMEM((2 * PAIRS, SUB, LANES), F32),
            pltpu.VMEM((2 * PAIRS, SUB, LANES), F32),
            pltpu.VMEM((2 * PAIRS, SUB, LANES), F32),
            pltpu.SMEM((3 * slots + 16,), jnp.int32),
        ],
        compiler_params=pltpu.CompilerParams(vmem_limit_bytes=60 * 1024 * 1024),
    )(codes, flags, as_tiles(guess), as_tiles(zlo), as_tiles(zhi), points, pay_lo, pay_hi)
    out = out.reshape(Z_DEV, Y_DEV // 8, SUB, 8, LANES).transpose(0, 1, 3, 2, 4)
    return out.reshape(Z_DEV, Y_DEV, NX)


def solution(mesh):
    placed = (
        P(("slab", "row"), None, None),
        P(("slab", "row"), None, None),
        P(("slab", "row"), None, None, None),
        P(("slab", "row"), None, None, None),
        P(("slab", "row"), None, None, None, None),
        P(("slab", "row"), None, None, None),
        P("slab", "row", None),
    )
    return jax.shard_map(
        shards, mesh=mesh, in_specs=placed, out_specs=P("slab", "row", None), check_vma=False
    )
```

```python
import functools
import jax
import jax.numpy as jnp
from jax import lax
from jax.experimental import pallas as pl
from jax.experimental.pallas import tpu as pltpu
from jax.sharding import PartitionSpec as P

Z_DEV = 16
Y_DEV = 16
NX = 1024
CAP = 64
S_PEER = 2
SWEEPS = 3
ALPHA = 4.0

HALO = 2 * SWEEPS
EXT = Z_DEV + 2 * HALO
PAIRS = EXT // 2
RIM = EXT + 2
LANES = 128
SUB = NX // LANES
CODE = 16384
UNROLL = 8
F32 = jnp.float32
BF16 = jnp.bfloat16


def chain(axis, step):
    size = lax.axis_size(axis)
    return [(i, i + step) for i in range(size) if 0 <= i + step < size]


def lane_sets():
    lane = lax.broadcasted_iota(jnp.int32, (SUB, LANES), 1)
    even = lane % 2 == 0
    return lane < CAP, (even, jnp.logical_not(even)), lane == 0, lane == LANES - 1


def find_places(pay, base, tiles, block, dy, entries):
    lane = lax.broadcasted_iota(jnp.int32, (8, LANES), 1)
    sub = lax.broadcasted_iota(jnp.int32, (8, LANES), 0)

    def find(i, _):
        brick = pay[pl.ds(base + i * 64 + 6, 8, stride=8), :].astype(jnp.int32) - 1
        t = i * 8 + sub
        dz = t - 3 * ((t * 21846) >> 16) - 1
        z = brick // Y_DEV + HALO + Z_DEV * dz
        y = brick % Y_DEV + HALO + Y_DEV * dy
        inside = (brick >= 0) & (z >= 0) & (z < EXT) & (y >= 0) & (y < EXT)
        row = block * tiles * S_PEER + (i * 2 + lane) * 8 + sub
        entry = ((z + 1) * RIM + y + 1) * CODE + row
        at = pl.multiple_of(block * tiles + i * 8, 8)
        entries[pl.ds(at, 8), :] = jnp.where(inside, entry, -1)
        return 0

    lax.fori_loop(0, tiles // 8, find, 0)


def prepare_points(pays, tiles, prep, places, todo):
    low = lane_sets()[0]
    slots = tiles * S_PEER
    group = 2
    dummy = (RIM + 1) * CODE + len(pays) * slots
    for u in range(UNROLL):
        todo[u] = jnp.int32(dummy)
    pos = jnp.int32(UNROLL)
    for block, (pay, base) in enumerate(pays):
        def prepare(i, pos, pay=pay, base=base, block=block):
            work = []
            for g in range(group):
                for s in range(S_PEER):
                    at = base + (i * group + g) * 64 + s
                    rows = [pay[pl.ds(at + 2 * r, 8, stride=8), :] for r in range(3)]
                    work.append((g, s, rows, [pltpu.roll(x, CAP, 1) for x in rows]))
            for k in range(8 * group):
                for s in range(S_PEER):
                    e = places[block * tiles + i * 8 * group + k, s]
                    todo[pos] = e
                    pos = pos + (e >= 0).astype(jnp.int32)
            for g, s, rows, turned in work:
                cell = jnp.where(low, rows[0], turned[0])
                frac = jnp.where(low, turned[0], rows[0])
                vals = []
                for r in (1, 2):
                    vals.append(jnp.where(low, rows[r], turned[r]))
                    vals.append(jnp.where(low, turned[r], rows[r]))
                less = 0.5 - frac
                more = 0.5 + frac
                weights = (
                    jnp.where(low, 0.5 * less * less, 0.75 - frac * frac),
                    jnp.where(low, 0.5 * more * more, 0.0),
                )
                whole = cell.astype(jnp.int32)
                at = pl.multiple_of(block * slots + ((i * group + g) * 2 + s) * 8, 8)
                for h in range(2):
                    c = jnp.where(low, whole - 1, whole) if h == 0 else whole + 1
                    prep[16 + h, pl.ds(at, 8), :] = (c >> 7).astype(F32)
                    prep[18 + h, pl.ds(at, 8), :] = (c & 127).astype(F32)
                    for ch in range(4):
                        v = vals[ch] * weights[h]
                        head = v.astype(BF16).astype(F32)
                        prep[h * 8 + ch, pl.ds(at, 8), :] = head
                        prep[h * 8 + 4 + ch, pl.ds(at, 8), :] = v - head
            return pos

        pos = lax.fori_loop(0, tiles // (8 * group), prepare, pos)
    zero = jnp.zeros((SUB, LANES), F32)
    for q in range(20):
        prep[q, pl.ds(len(pays) * slots, 8), :] = zero
    for u in range(UNROLL):
        todo[pos + u] = jnp.int32(dummy)
    return pos - UNROLL


def splat_slots(count, todo, prep, stage, accd, accr):
    sub = lax.broadcasted_iota(jnp.int32, (SUB, LANES), 0)
    subf = sub.astype(F32)
    keep_up = (sub > 0).astype(F32)
    keep_dn = (sub < SUB - 1).astype(F32)
    first_lane, last_lane = lane_sets()[2:]
    col = lax.broadcasted_iota(jnp.int32, (LANES, LANES), 0).astype(F32).astype(BF16)
    one = jnp.ones((LANES, LANES), BF16)
    nil = jnp.zeros((LANES, LANES), BF16)
    for q in range(4 * UNROLL):
        stage[q] = jnp.zeros((SUB, LANES), F32)

    def add(i):
        slopes = []
        for u in range(UNROLL):
            v = stage[4 * u]
            up = jnp.where(last_lane, pltpu.roll(v, 1, 0) * keep_up, v)
            dn = jnp.where(first_lane, pltpu.roll(v, SUB - 1, 0) * keep_dn, v)
            slopes.append(pltpu.roll(dn, LANES - 1, 1) - pltpu.roll(up, 1, 1))
        for u in range(UNROLL):
            centre = todo[i * UNROLL + u] // CODE
            f1, f2, f3 = (stage[4 * u + ch] for ch in range(1, 4))
            new = [
                accd[centre] + f3,
                accr[centre] + slopes[u],
                accr[centre + 1] + f1,
                accr[centre - 1] - f1,
                accr[centre + RIM] + f2,
                accr[centre - RIM] - f2,
            ]
            accd[centre] = new[0]
            accr[centre] = new[1]
            accr[centre + 1] = new[2]
            accr[centre - 1] = new[3]
            accr[centre + RIM] = new[4]
            accr[centre - RIM] = new[5]

    def splat(i, _):
        add(i)
        sums = []
        for u in range(UNROLL):
            row = todo[(i + 1) * UNROLL + u] % CODE
            lhs, rhs = [], []
            for h in range(2):
                hi = jnp.broadcast_to(prep[16 + h, pl.ds(row, 1), :], (SUB, LANES))
                hit = hi == subf
                parts = [
                    jnp.where(hit, jnp.broadcast_to(prep[h * 8 + q, pl.ds(row, 1), :], (SUB, LANES)), 0.0)
                    for q in range(8)
                ]
                lhs.append(jnp.concatenate(parts, axis=0))
                lo = jnp.broadcast_to(prep[18 + h, pl.ds(row, 1), :], (LANES, LANES)).astype(BF16)
                rhs.append(jnp.where(lo == col, one, nil))
            left = jnp.concatenate(lhs, axis=1).astype(BF16)
            right = jnp.concatenate(rhs, axis=1)
            res = lax.dot_general(left, right, (((1,), (1,)), ((), ())), preferred_element_type=F32)
            sums.append([res[ch * 8:ch * 8 + 8] + res[32 + ch * 8:40 + ch * 8] for ch in range(4)])
        for u in range(UNROLL):
            for ch in range(4):
                stage[4 * u + ch] = sums[u][ch]
        return 0

    groups = (count + UNROLL - 1) // UNROLL
    lax.fori_loop(0, groups, splat, 0)
    add(groups)


def at_row(z, j):
    return pl.ds((z * PAIRS + j) * 9 + 1, SUB)


def pack_pair(vr, vb, z, j, m, a, b):
    vr[at_row(z, j), :] = jnp.where(m, a, b)
    vb[at_row(z, j), :] = jnp.where(m, b, a)


def side_sums(v, z, pairs):
    first_lane, last_lane = lane_sets()[2:]
    res = []
    for j in pairs:
        at = (z * PAIRS + j) * 9
        x = v[pl.ds(at + 1, SUB), :]
        up = jnp.where(last_lane, v[pl.ds(at, SUB), :], x)
        dn = jnp.where(first_lane, v[pl.ds(at + 2, SUB), :], x)
        res.append((j, pltpu.roll(up, 1, 1) + pltpu.roll(dn, LANES - 1, 1)))
    return res


def keep_sums(sums, z, res):
    for j, value in res:
        sums[z * PAIRS + j] = value


def near_kernel(tiles, guess, zlo, zhi, ylo, yhi, points, accd, accr, vr, vb, sr,
                prep, stage, todo, entries, places, sem):
    zero = jnp.zeros((SUB, LANES), F32)
    par = lane_sets()[1]
    find_places(points, 0, tiles, 0, 0, entries)
    fetch = pltpu.make_async_copy(entries, places, sem.at[0])
    fetch.start()

    def clear(i, _):
        for u in range(12):
            accd[i * 12 + u] = zero
            accr[i * 12 + u] = zero
        return 0

    lax.fori_loop(0, RIM * RIM // 12, clear, 0)

    def clear_v(i, _):
        for u in range(9):
            vr[pl.ds(i * 72 + u * 8, 8), :] = zero
            vb[pl.ds(i * 72 + u * 8, 8), :] = zero
        return 0

    lax.fori_loop(0, vr.shape[0] // 72, clear_v, 0)
    fetch.wait()
    count = prepare_points(((points, 0),), tiles, prep, places, todo)
    splat_slots(count, todo, prep, stage, accd, accr)

    def edges(i, _):
        for u in range(2):
            for src, z0 in ((zlo, 0), (zhi, HALO + Z_DEV)):
                zi = i * 2 + u
                for j in range(Y_DEV // 2):
                    a = src[zi, 2 * j // 8, pl.ds(2 * j % 8, 8, stride=8), :]
                    b = src[zi, 2 * j // 8, pl.ds(2 * j % 8 + 1, 8, stride=8), :]
                    pack_pair(vr, vb, z0 + zi, HALO // 2 + j, par[u], a, b)
        return 0

    def middle(i, _):
        for u in range(2):
            zi = i * 2 + u
            for j in range(Y_DEV // 2):
                a = guess[zi, 2 * j // 8, pl.ds(2 * j % 8, 8, stride=8), :]
                b = guess[zi, 2 * j // 8, pl.ds(2 * j % 8 + 1, 8, stride=8), :]
                pack_pair(vr, vb, HALO + zi, HALO // 2 + j, par[u], a, b)
            for j in range(HALO // 2):
                y = 8 - HALO + 2 * j
                a, b = (ylo[zi, pl.ds(y + k, 8, stride=8), :] for k in range(2))
                pack_pair(vr, vb, HALO + zi, j, par[u], a, b)
                a, b = (yhi[zi, pl.ds(2 * j + k, 8, stride=8), :] for k in range(2))
                pack_pair(vr, vb, HALO + zi, (HALO + Y_DEV) // 2 + j, par[u], a, b)
        return 0

    lax.fori_loop(0, HALO // 2, edges, 0)
    lax.fori_loop(0, Z_DEV // 2, middle, 0)

    def first_sums(i, _):
        for u in range(2):
            keep_sums(sr, i * 2 + u, side_sums(vr, i * 2 + u, range(PAIRS)))
        return 0

    lax.fori_loop(0, EXT // 2, first_sums, 0)


def relax_kernel(tiles, flags, pay_lo, pay_hi, *refs):
    accd, accr, vr, vb, sr, out = refs[5:11]
    prep, stage, gr, gb, ir, ib, sb, qa, todo, entries, places, sem = refs[11:]
    par = lane_sets()[1]
    zero = jnp.zeros((SUB, LANES), F32)
    base = 2 * HALO * HALO * SUB
    pays = ((pay_lo, base), (pay_hi, base))
    find_places(pay_lo, base, tiles, 0, -1, entries)
    find_places(pay_hi, base, tiles, 1, 1, entries)
    fetch = pltpu.make_async_copy(entries, places, sem.at[0])
    fetch.start()

    edge_pairs = (*range(HALO // 2), *range((HALO + Y_DEV) // 2, PAIRS))

    def corners(i, _):
        for half in range(2):
            for u in range(2):
                zi = half * HALO + i * 2 + u
                z = zi + half * Z_DEV
                for j in range(HALO // 2):
                    for pay, j0 in ((pay_lo, 0), (pay_hi, (HALO + Y_DEV) // 2)):
                        a, b = (pay[pl.ds((zi * HALO + 2 * j + k) * SUB, SUB), :] for k in range(2))
                        pack_pair(vr, vb, z, j0 + j, par[u], a, b)
        for half in range(2):
            for u in range(2):
                z = half * (HALO + Z_DEV) + i * 2 + u
                keep_sums(sr, z, side_sums(vr, z, edge_pairs))
        return 0

    lax.fori_loop(0, HALO // 2, corners, 0)
    fetch.wait()
    count = prepare_points(pays, tiles, prep, places, todo)
    splat_slots(count, todo, prep, stage, accd, accr)

    at_zlo, at_zhi, at_ylo, at_yhi = (flags[k] for k in range(4))

    def finish(i, _):
        for u in range(2):
            z = 1 + i * 2 + u
            m = par[(1 + u) % 2]
            fz = jnp.where(z < HALO, at_zlo, jnp.where(z >= HALO + Z_DEV, at_zhi, 1))
            for j in range(PAIRS):
                fy = at_ylo if j < HALO // 2 else at_yhi if j >= (HALO + Y_DEV) // 2 else None
                f = fz if fy is None else fz * fy
                scale = jnp.broadcast_to(f.astype(F32) * (1.0 / 6.0), (SUB, LANES))
                r = (z + 1) * RIM + 2 * j + 1
                da, db = accd[r], accd[r + 1]
                ra, rb = accr[r], accr[r + 1]
                at = z * PAIRS + j
                ir[at] = scale / (8.0 / 3.0 + ALPHA * jnp.where(m, da, db))
                ib[at] = scale / (8.0 / 3.0 + ALPHA * jnp.where(m, db, da))
                gr[at] = jnp.where(m, ra, rb)
                gb[at] = jnp.where(m, rb, ra)
        return 0

    lax.fori_loop(0, (EXT - 2) // 2, finish, 0)

    def pairs_of(k):
        return [j for j in range(k // 2 - 1, PAIRS + 1 - k // 2) if 0 <= j < PAIRS]

    def arrays_of(k):
        return (vr, vb, sr, sb, gr, ir) if k % 2 else (vb, vr, sb, sr, gb, ib)

    def advance(k, p, pp, update, mid):
        vx, _, sums, others, gx, ix = arrays_of(k)
        m = par[((k - 1) % 2 + pp) % 2]
        s, t = {}, {}
        for j in pairs_of(k):
            s[j] = sums[p * PAIRS + j]
            t[j] = vx[at_row(p, j), :] + 0.5 * others[p * PAIRS + j]
        for j in range(k // 2, PAIRS - k // 2):
            q = s[j] + t[j] + jnp.where(m, t.get(j + 1, zero), t.get(j - 1, zero))
            if update:
                at = (p - 1) * PAIRS + j
                vx[at_row(p - 1, j), :] = ix[at] * (gx[at] + (qa[PAIRS + j] + q))
            if mid:
                qa[PAIRS + j] = s[j] + jnp.where(m, s.get(j - 1, zero), s.get(j + 1, zero)) + qa[j]
            qa[j] = q

    def sides(k, p):
        return side_sums(arrays_of(k)[1], p, pairs_of(k))

    def keep(k, p, res):
        keep_sums(arrays_of(k)[3], p, res)

    for p in range(2):
        keep(1, p, sides(1, p))
    for k in range(1, HALO + 1):
        first = k - 1
        ahead = [sides(k, first + 2 + u) for u in range(2)]
        advance(k, first, first, False, False)
        advance(k, first + 1, first + 1, False, True)
        for u in range(2):
            keep(k, first + 2 + u, ahead[u])
        steps = (EXT - 2 * k) // 2

        def body(i, _, k=k, first=first):
            p = first + 2 + i * 2
            ahead = [sides(k, p + 2 + u) for u in range(2)]
            advance(k, p, first, True, True)
            advance(k, p + 1, first + 1, True, True)
            for u in range(2):
                keep(k, p + 2 + u, ahead[u])
            return 0

        lax.fori_loop(0, steps - 1, body, 0)
        p = first + 2 * steps
        ahead = [sides(k + 1, k + u) for u in range(2)] if k < HALO else []
        advance(k, p, first, True, True)
        advance(k, p + 1, first + 1, True, False)
        for u, res in enumerate(ahead):
            keep(k + 1, k + u, res)

    def unpack(i, _):
        for u in range(2):
            z = HALO + i * 2 + u
            m = par[u]
            for j in range(HALO // 2, (HALO + Y_DEV) // 2):
                r, b = vr[at_row(z, j), :], vb[at_row(z, j), :]
                y = 2 * j - HALO
                out[i * 2 + u, y // 8, pl.ds(y % 8, 8, stride=8), :] = jnp.where(m, r, b)
                out[i * 2 + u, y // 8, pl.ds(y % 8 + 1, 8, stride=8), :] = jnp.where(m, b, r)
        return 0

    lax.fori_loop(0, Z_DEV // 2, unpack, 0)


def corner_kernel(zlo, zhi, points, top, bottom):
    for half, src in enumerate((zlo, zhi)):
        def corner(z, _, half=half, src=src):
            for y in range(HALO):
                at = pl.ds(((half * HALO + z) * HALO + y) * SUB, SUB)
                top[at, :] = src[z, Y_DEV // 8 - 1, pl.ds(8 - HALO + y, 8, stride=8), :]
                bottom[at, :] = src[z, 0, pl.ds(y, 8, stride=8), :]
            return 0

        lax.fori_loop(0, HALO, corner, 0)
    base = 2 * HALO * HALO * SUB

    def copy(i, _):
        for u in range(8):
            block = points[pl.ds(i * 64 + u * 8, 8), :]
            top[pl.ds(base + i * 64 + u * 8, 8), :] = block
            bottom[pl.ds(base + i * 64 + u * 8, 8), :] = block
        return 0

    lax.fori_loop(0, points.shape[0] // 64, copy, 0)


def as_tiles(a):
    d = a.shape[0]
    a = a.reshape(d, Y_DEV // 8, 8, SUB, LANES).transpose(0, 1, 3, 2, 4)
    return a.reshape(d, Y_DEV // 8, 8 * SUB, LANES)


def shards(slot_brick, slot_count, point_cell, point_frac, point_normal, point_weight, guess):
    n_slab, n_row = lax.axis_size("slab"), lax.axis_size("row")
    peers = point_cell.shape[1]
    tiles = 3 * peers
    slots = tiles * S_PEER

    lanes = jnp.arange(CAP, dtype=jnp.int32)
    live = (lanes < slot_count[0][:, :, None]).astype(F32)
    n = point_normal[0]
    rows0 = jnp.concatenate([point_cell[0].astype(F32), point_frac[0]], axis=-1)
    rows1 = jnp.concatenate([n[:, :, 0] * (-3.0 * live), n[:, :, 1] * (3.0 * live)], axis=-1)
    rows2 = jnp.concatenate([n[:, :, 2] * (3.0 * live), point_weight[0] * live], axis=-1)
    brick = jnp.pad((slot_brick[0] + 1).astype(F32)[:, None, :], ((0, 0), (0, 1), (0, LANES - S_PEER)))
    tile = jnp.concatenate([rows0, rows1, rows2, brick], axis=1).reshape(n_slab, n_row, 8, LANES)
    gap = jnp.zeros((1, n_row, 8, LANES), F32)
    below = jnp.concatenate([gap, tile[:-1]], axis=0)
    above = jnp.concatenate([tile[1:], gap], axis=0)
    send = jnp.stack([below, tile, above], axis=2).reshape(peers, 3, 8, LANES)

    zlo = lax.ppermute(guess[Z_DEV - HALO:], "slab", chain("slab", 1))
    zhi = lax.ppermute(guess[:HALO], "slab", chain("slab", -1))
    got = lax.all_to_all(send, ("slab", "row"), split_axis=0, concat_axis=0, tiled=True)
    split = as_tiles(guess)
    ylo = lax.ppermute(split[:, -1], "row", chain("row", 1))
    yhi = lax.ppermute(split[:, 0], "row", chain("row", -1))
    points = got.reshape(tiles * 8, LANES)
    zlo, zhi = as_tiles(zlo), as_tiles(zhi)

    vmem = pl.BlockSpec(memory_space=pltpu.VMEM)
    smem = pl.BlockSpec(memory_space=pltpu.SMEM)
    packed = pltpu.VMEM((EXT * PAIRS, SUB, LANES), F32)
    pay = jax.ShapeDtypeStruct((2 * HALO * HALO * SUB + tiles * 8, LANES), F32)
    top, bottom = pl.pallas_call(
        corner_kernel,
        out_shape=(pay, pay),
        in_specs=[vmem] * 3,
        out_specs=[vmem] * 2,
        compiler_params=pltpu.CompilerParams(vmem_limit_bytes=8 * 1024 * 1024),
    )(zlo, zhi, points)
    pay_lo = lax.ppermute(top, "row", chain("row", 1))
    pay_hi = lax.ppermute(bottom, "row", chain("row", -1))
    zi, yi = lax.axis_index("slab"), lax.axis_index("row")
    flags = jnp.stack([zi > 0, zi < n_slab - 1, yi > 0, yi < n_row - 1]).astype(jnp.int32)

    cells = RIM * RIM
    state = (
        jax.ShapeDtypeStruct((cells, SUB, LANES), F32),
        jax.ShapeDtypeStruct((cells, SUB, LANES), F32),
        jax.ShapeDtypeStruct(((EXT * PAIRS * 9 + 8 + 71) // 72 * 72, LANES), F32),
        jax.ShapeDtypeStruct(((EXT * PAIRS * 9 + 8 + 71) // 72 * 72, LANES), F32),
        jax.ShapeDtypeStruct((EXT * PAIRS, SUB, LANES), F32),
    )

    def lists(blocks):
        return [
            pltpu.SMEM((blocks * slots + 2 * UNROLL,), jnp.int32),
            pltpu.VMEM((blocks * tiles, LANES), jnp.int32),
            pltpu.SMEM((blocks * tiles, LANES), jnp.int32),
            pltpu.SemaphoreType.DMA((1,)),
        ]

    def limit(blocks, extra):
        return (extra << 20) + 20 * blocks * slots * LANES * 4

    held = pl.pallas_call(
        functools.partial(near_kernel, tiles),
        out_shape=state,
        in_specs=[vmem] * 6,
        out_specs=[vmem] * 5,
        scratch_shapes=[
            pltpu.VMEM((20, slots + 8, LANES), F32),
            pltpu.VMEM((4 * UNROLL, SUB, LANES), F32),
        ] + lists(1),
        cost_estimate=pl.CostEstimate(flops=40_000_000_000, bytes_accessed=1_000_000, transcendentals=0),
        compiler_params=pltpu.CompilerParams(vmem_limit_bytes=limit(1, 6)),
    )(split, zlo, zhi, ylo, yhi, points)
    out = pl.pallas_call(
        functools.partial(relax_kernel, tiles),
        out_shape=state + (jax.ShapeDtypeStruct((Z_DEV, Y_DEV // 8, 8 * SUB, LANES), F32),),
        in_specs=[smem] + [vmem] * 7,
        out_specs=[vmem] * 6,
        input_output_aliases={3 + i: i for i in range(5)},
        scratch_shapes=[
            pltpu.VMEM((20, 2 * slots + 8, LANES), F32),
            pltpu.VMEM((4 * UNROLL, SUB, LANES), F32),
            packed, packed, packed, packed, packed,
            pltpu.VMEM((2 * PAIRS, SUB, LANES), F32),
        ] + lists(2),
        compiler_params=pltpu.CompilerParams(vmem_limit_bytes=limit(2, 16)),
    )(flags, pay_lo, pay_hi, *held)[-1]
    out = out.reshape(Z_DEV, Y_DEV // 8, SUB, 8, LANES).transpose(0, 1, 3, 2, 4)
    return out.reshape(Z_DEV, Y_DEV, NX)


def solution(mesh):
    placed = (
        P(("slab", "row"), None, None),
        P(("slab", "row"), None, None),
        P(("slab", "row"), None, None, None),
        P(("slab", "row"), None, None, None),
        P(("slab", "row"), None, None, None, None),
        P(("slab", "row"), None, None, None),
        P("slab", "row", None),
    )
    return jax.shard_map(
        shards, mesh=mesh, in_specs=placed, out_specs=P("slab", "row", None), check_vma=False
    )
```

```python
import functools
import jax
import jax.numpy as jnp
from jax import lax
from jax.experimental import pallas as pl
from jax.experimental.pallas import tpu as pltpu
from jax.sharding import PartitionSpec as P

Z_DEV = 16
Y_DEV = 16
NX = 1024
CAP = 64
S_PEER = 2
SWEEPS = 3
ALPHA = 4.0

HALO = 2 * SWEEPS
EXT = Z_DEV + 2 * HALO
PAIRS = EXT // 2
RIM = EXT + 2
LANES = 128
SUB = NX // LANES
CODE = 16384
UNROLL = 16
F32 = jnp.float32
BF16 = jnp.bfloat16


def chain(axis, step):
    size = lax.axis_size(axis)
    return [(i, i + step) for i in range(size) if 0 <= i + step < size]


def swaps(axis, start):
    pairs = [(i, i + 1) for i in range(start, lax.axis_size(axis) - 1, 2)]
    return pairs + [(j, i) for i, j in pairs]


def lane_sets():
    lane = lax.broadcasted_iota(jnp.int32, (SUB, LANES), 1)
    even = lane % 2 == 0
    return lane < CAP, (even, jnp.logical_not(even)), lane == 0, lane == LANES - 1


def find_places(pay, base, tiles, block, dy, entries):
    lane = lax.broadcasted_iota(jnp.int32, (8, LANES), 1)
    sub = lax.broadcasted_iota(jnp.int32, (8, LANES), 0)

    def find(i, _):
        brick = pay[pl.ds(base + i * 64 + 6, 8, stride=8), :].astype(jnp.int32) - 1
        t = i * 8 + sub
        dz = t - 3 * ((t * 21846) >> 16) - 1
        z = brick // Y_DEV + HALO + Z_DEV * dz
        y = brick % Y_DEV + HALO + Y_DEV * dy
        inside = (brick >= 0) & (z >= 0) & (z < EXT) & (y >= 0) & (y < EXT)
        row = block * tiles * S_PEER + (i * 2 + lane) * 8 + sub
        entry = ((z + 1) * RIM + y + 1) * CODE + row
        at = pl.multiple_of(block * tiles + i * 8, 8)
        entries[pl.ds(at, 8), :] = jnp.where(inside, entry, -1)
        return 0

    lax.fori_loop(0, tiles // 8, find, 0)


def prepare_points(pays, tiles, prep, places, todo):
    low = lane_sets()[0]
    slots = tiles * S_PEER
    group = 2
    dummy = (RIM + 1) * CODE + len(pays) * slots
    for u in range(UNROLL):
        todo[u] = jnp.int32(dummy)
    pos = jnp.int32(UNROLL)
    for block, (pay, base) in enumerate(pays):
        def prepare(i, pos, pay=pay, base=base, block=block):
            work = []
            for g in range(group):
                for s in range(S_PEER):
                    at = base + (i * group + g) * 64 + s
                    rows = [pay[pl.ds(at + 2 * r, 8, stride=8), :] for r in range(3)]
                    work.append((g, s, rows, [pltpu.roll(x, CAP, 1) for x in rows]))
            for half in range(group):
                found = [
                    places[block * tiles + (i * group + half) * 8 + k, s] for k in range(8) for s in range(S_PEER)
                ]
                for e in found:
                    todo[pos] = e
                    pos = pos + (1 + (e >> 31))
            for g, s, rows, turned in work:
                cell = jnp.where(low, rows[0], turned[0])
                frac = jnp.where(low, turned[0], rows[0])
                vals = []
                for r in (1, 2):
                    vals.append(jnp.where(low, rows[r], turned[r]))
                    vals.append(jnp.where(low, turned[r], rows[r]))
                less = 0.5 - frac
                more = 0.5 + frac
                weights = (
                    jnp.where(low, 0.5 * less * less, 0.75 - frac * frac),
                    jnp.where(low, 0.5 * more * more, 0.0),
                )
                whole = cell.astype(jnp.int32)
                at = pl.multiple_of(block * slots + ((i * group + g) * 2 + s) * 8, 8)
                for h in range(2):
                    c = jnp.where(low, whole - 1, whole) if h == 0 else whole + 1
                    prep[16 + h, pl.ds(at, 8), :] = (c >> 7).astype(F32)
                    prep[18 + h, pl.ds(at, 8), :] = (c & 127).astype(F32)
                    for ch in range(4):
                        v = vals[ch] * weights[h]
                        head = v.astype(BF16).astype(F32)
                        prep[h * 8 + ch, pl.ds(at, 8), :] = head
                        prep[h * 8 + 4 + ch, pl.ds(at, 8), :] = v - head
            return pos

        pos = lax.fori_loop(0, tiles // (8 * group), prepare, pos)
    zero = jnp.zeros((SUB, LANES), F32)
    for q in range(20):
        prep[q, pl.ds(len(pays) * slots, 8), :] = zero
    for u in range(UNROLL):
        todo[pos + u] = jnp.int32(dummy)
    return pos - UNROLL


def splat_slots(count, todo, prep, stage, accd, accr):
    sub = lax.broadcasted_iota(jnp.int32, (SUB, LANES), 0)
    subf = sub.astype(F32)
    keep_up = (sub > 0).astype(F32)
    keep_dn = (sub < SUB - 1).astype(F32)
    first_lane, last_lane = lane_sets()[2:]
    col = lax.broadcasted_iota(jnp.int32, (LANES, LANES), 0).astype(F32).astype(BF16)
    one = jnp.ones((LANES, LANES), BF16)
    nil = jnp.zeros((LANES, LANES), BF16)
    for q in range(4 * UNROLL):
        stage[q] = jnp.zeros((SUB, LANES), F32)

    def add(i):
        slopes = []
        for u in range(UNROLL):
            v = stage[4 * u]
            up = jnp.where(last_lane, pltpu.roll(v, 1, 0) * keep_up, v)
            dn = jnp.where(first_lane, pltpu.roll(v, SUB - 1, 0) * keep_dn, v)
            slopes.append(pltpu.roll(dn, LANES - 1, 1) - pltpu.roll(up, 1, 1))
        for u in range(UNROLL):
            centre = todo[i * UNROLL + u] >> 14
            f1, f2, f3 = (stage[4 * u + ch] for ch in range(1, 4))
            new = [
                accd[centre] + f3,
                accr[centre] + slopes[u],
                accr[centre + 1] + f1,
                accr[centre - 1] - f1,
                accr[centre + RIM] + f2,
                accr[centre - RIM] - f2,
            ]
            accd[centre] = new[0]
            accr[centre] = new[1]
            accr[centre + 1] = new[2]
            accr[centre - 1] = new[3]
            accr[centre + RIM] = new[4]
            accr[centre - RIM] = new[5]

    def splat(i, _):
        add(i)
        sums = []
        for u in range(UNROLL):
            row = todo[(i + 1) * UNROLL + u] & (CODE - 1)
            lhs, rhs = [], []
            for h in range(2):
                hi = jnp.broadcast_to(prep[16 + h, pl.ds(row, 1), :], (SUB, LANES))
                hit = hi == subf
                parts = [
                    jnp.where(hit, jnp.broadcast_to(prep[h * 8 + q, pl.ds(row, 1), :], (SUB, LANES)), 0.0)
                    for q in range(8)
                ]
                lhs.append(jnp.concatenate(parts, axis=0))
                lo = jnp.broadcast_to(prep[18 + h, pl.ds(row, 1), :], (LANES, LANES)).astype(BF16)
                rhs.append(jnp.where(lo == col, one, nil))
            left = jnp.concatenate(lhs, axis=1).astype(BF16)
            right = jnp.concatenate(rhs, axis=1)
            res = lax.dot_general(left, right, (((1,), (1,)), ((), ())), preferred_element_type=F32)
            sums.append([res[ch * 8:ch * 8 + 8] + res[32 + ch * 8:40 + ch * 8] for ch in range(4)])
        for u in range(UNROLL):
            for ch in range(4):
                stage[4 * u + ch] = sums[u][ch]
        return 0

    groups = (count + UNROLL - 1) // UNROLL
    lax.fori_loop(0, groups, splat, 0)
    add(groups)


def at_row(z, j):
    return pl.ds((z * PAIRS + j) * 9 + 1, SUB)


def pack_pair(vr, vb, z, j, m, a, b):
    vr[at_row(z, j), :] = jnp.where(m, a, b)
    vb[at_row(z, j), :] = jnp.where(m, b, a)


def side_sums(v, z, pairs):
    first_lane, last_lane = lane_sets()[2:]
    res = []
    for j in pairs:
        at = (z * PAIRS + j) * 9
        x = v[pl.ds(at + 1, SUB), :]
        up = jnp.where(last_lane, v[pl.ds(at, SUB), :], x)
        dn = jnp.where(first_lane, v[pl.ds(at + 2, SUB), :], x)
        res.append((j, pltpu.roll(up, 1, 1) + pltpu.roll(dn, LANES - 1, 1)))
    return res


def keep_sums(sums, z, res):
    for j, value in res:
        sums[z * PAIRS + j] = value


def deal_kernel(n_row, brick_in, number_in, guess, cell_in, frac_in, normal_in, weight_in, send, low_planes, high_planes,
                brick, number, cell, frac, normal, weight, sem):
    moves = [
        pltpu.make_async_copy(guess.at[pl.ds(0, HALO)], low_planes, sem.at[0]),
        pltpu.make_async_copy(guess.at[pl.ds(Z_DEV - HALO, HALO)], high_planes, sem.at[1]),
    ]
    pairs = ((brick_in, brick), (number_in, number), (cell_in, cell), (frac_in, frac), (normal_in, normal),
             (weight_in, weight))
    loads = [pltpu.make_async_copy(src, dst, sem.at[2 + i]) for i, (src, dst) in enumerate(pairs)]
    for move in loads + moves:
        move.start()
    peers = cell.shape[0]
    lane = lax.broadcasted_iota(jnp.int32, (S_PEER, CAP), 1)
    sub = lax.broadcasted_iota(jnp.int32, (S_PEER, CAP), 0)
    wide = lax.broadcasted_iota(jnp.int32, (2, LANES), 1)
    top = lax.broadcasted_iota(jnp.int32, (2, LANES), 0) == 0
    empty = jnp.zeros((8, LANES), F32)
    for d in range(n_row):
        send[d, 0] = empty
        send[peers - 1 - d, 2] = empty
    for move in loads:
        move.wait()
    group = 4

    def tile(i, _):
        for g in range(group):
            d = i * group + g
            live = (lane < jnp.where(sub == 0, number[0, d], number[1, d])).astype(F32)
            first = brick[0, d] + 1
            second = brick[1, d] + 1
            place = jnp.where(wide == 0, first, jnp.where(wide == 1, second, 0))
            place = jnp.where(top, place, 0).astype(F32)
            pieces = (
                jnp.concatenate([cell[d].astype(F32), frac[d]], axis=1),
                jnp.concatenate([normal[d, 0] * (-3.0 * live), normal[d, 1] * (3.0 * live)], axis=1),
                jnp.concatenate([normal[d, 2] * (3.0 * live), weight[d] * live], axis=1),
                place,
            )
            for r, piece in enumerate(pieces):
                send[d, 1, 2 * r:2 * r + 2, :] = piece
        return 0

    lax.fori_loop(0, peers // group, tile, 0)

    def spread(i, _):
        for g in range(group):
            d = i * group + g
            block = send[d, 1]
            below = send[d + n_row, 1]
            send[d + n_row, 0] = block
            send[d, 2] = below
        return 0

    lax.fori_loop(0, (peers - n_row) // group, spread, 0)
    for move in moves:
        move.wait()


def near_kernel(tiles, guess, zlo, zhi, ylo, yhi, points, accd, accr, vr, vb, sr,
                prep, stage, todo, entries, places, sem):
    zero = jnp.zeros((SUB, LANES), F32)
    par = lane_sets()[1]
    find_places(points, 0, tiles, 0, 0, entries)
    fetch = pltpu.make_async_copy(entries, places, sem.at[0])
    fetch.start()

    def clear(i, _):
        for u in range(12):
            accd[i * 12 + u] = zero
            accr[i * 12 + u] = zero
        return 0

    lax.fori_loop(0, RIM * RIM // 12, clear, 0)

    def clear_v(i, _):
        for u in range(9):
            vr[pl.ds(i * 72 + u * 8, 8), :] = zero
            vb[pl.ds(i * 72 + u * 8, 8), :] = zero
        return 0

    lax.fori_loop(0, vr.shape[0] // 72, clear_v, 0)

    def edges(i, _):
        for u in range(2):
            for src, z0 in ((zlo, 0), (zhi, HALO + Z_DEV)):
                zi = i * 2 + u
                for j in range(Y_DEV // 2):
                    a = src[zi, 2 * j // 8, pl.ds(2 * j % 8, 8, stride=8), :]
                    b = src[zi, 2 * j // 8, pl.ds(2 * j % 8 + 1, 8, stride=8), :]
                    pack_pair(vr, vb, z0 + zi, HALO // 2 + j, par[u], a, b)
        return 0

    def middle(i, _):
        for u in range(2):
            zi = i * 2 + u
            for j in range(Y_DEV // 2):
                a = guess[zi, 2 * j // 8, pl.ds(2 * j % 8, 8, stride=8), :]
                b = guess[zi, 2 * j // 8, pl.ds(2 * j % 8 + 1, 8, stride=8), :]
                pack_pair(vr, vb, HALO + zi, HALO // 2 + j, par[u], a, b)
            for j in range(HALO // 2):
                y = 8 - HALO + 2 * j
                a, b = (ylo[zi, pl.ds(y + k, 8, stride=8), :] for k in range(2))
                pack_pair(vr, vb, HALO + zi, j, par[u], a, b)
                a, b = (yhi[zi, pl.ds(2 * j + k, 8, stride=8), :] for k in range(2))
                pack_pair(vr, vb, HALO + zi, (HALO + Y_DEV) // 2 + j, par[u], a, b)
        return 0

    lax.fori_loop(0, HALO // 2, edges, 0)
    lax.fori_loop(0, Z_DEV // 2, middle, 0)

    def first_sums(i, _):
        res = [side_sums(vr, i * 4 + u, range(PAIRS)) for u in range(4)]
        for u in range(4):
            keep_sums(sr, i * 4 + u, res[u])
        return 0

    lax.fori_loop(0, EXT // 4, first_sums, 0)
    fetch.wait()
    count = prepare_points(((points, 0),), tiles, prep, places, todo)
    splat_slots(count, todo, prep, stage, accd, accr)


def relax_kernel(tiles, flags, pay_outer, pay_inner, *refs):
    accd, accr, vr, vb, sr, out = refs[5:11]
    prep, stage, gr, gb, ir, ib, sb, qa, held, out_sem, todo, entries, places, sem = refs[11:]
    par = lane_sets()[1]
    zero = jnp.zeros((SUB, LANES), F32)
    base = 2 * HALO * HALO * SUB
    pays = ((pay_outer, base), (pay_inner, base))
    at_zlo, at_zhi, at_ylo, at_yhi, odd = (flags[k] for k in range(5))
    side = 2 * odd - 1
    find_places(pay_outer, base, tiles, 0, side, entries)
    find_places(pay_inner, base, tiles, 1, -side, entries)
    high = (HALO + Y_DEV) // 2
    fetch = pltpu.make_async_copy(entries, places, sem.at[0])
    fetch.start()

    edge_pairs = (*range(HALO // 2), *range((HALO + Y_DEV) // 2, PAIRS))

    def corners(i, _):
        for half in range(2):
            for u in range(2):
                zi = half * HALO + i * 2 + u
                z = zi + half * Z_DEV
                for j in range(HALO // 2):
                    for pay, j0 in ((pay_outer, high * odd), (pay_inner, high * (1 - odd))):
                        a, b = (pay[pl.ds((zi * HALO + 2 * j + k) * SUB, SUB), :] for k in range(2))
                        pack_pair(vr, vb, z, j0 + j, par[u], a, b)
        for half in range(2):
            for u in range(2):
                z = half * (HALO + Z_DEV) + i * 2 + u
                keep_sums(sr, z, side_sums(vr, z, edge_pairs))
        return 0

    lax.fori_loop(0, HALO // 2, corners, 0)
    fetch.wait()
    count = prepare_points(pays, tiles, prep, places, todo)
    splat_slots(count, todo, prep, stage, accd, accr)

    def finish(i, _):
        for u in range(2):
            z = 1 + i * 2 + u
            m = par[(1 + u) % 2]
            fz = jnp.where(z < HALO, at_zlo, jnp.where(z >= HALO + Z_DEV, at_zhi, 1))
            for j in range(PAIRS):
                fy = at_ylo if j < HALO // 2 else at_yhi if j >= (HALO + Y_DEV) // 2 else None
                f = fz if fy is None else fz * fy
                scale = jnp.broadcast_to(f.astype(F32) * (1.0 / 6.0), (SUB, LANES))
                r = (z + 1) * RIM + 2 * j + 1
                da, db = accd[r], accd[r + 1]
                ra, rb = accr[r], accr[r + 1]
                at = z * PAIRS + j
                ir[at] = scale / (8.0 / 3.0 + ALPHA * jnp.where(m, da, db))
                ib[at] = scale / (8.0 / 3.0 + ALPHA * jnp.where(m, db, da))
                gr[at] = jnp.where(m, ra, rb)
                gb[at] = jnp.where(m, rb, ra)
        return 0

    lax.fori_loop(0, (EXT - 2) // 2, finish, 0)

    def pairs_of(k):
        return [j for j in range(k // 2 - 1, PAIRS + 1 - k // 2) if 0 <= j < PAIRS]

    def arrays_of(k):
        return (vr, vb, sr, sb, gr, ir) if k % 2 else (vb, vr, sb, sr, gb, ib)

    def advance(k, p, pp, update, mid):
        vx, _, sums, others, gx, ix = arrays_of(k)
        m = par[((k - 1) % 2 + pp) % 2]
        s, t = {}, {}
        for j in pairs_of(k):
            s[j] = sums[p * PAIRS + j]
            t[j] = vx[at_row(p, j), :] + 0.5 * others[p * PAIRS + j]
        for j in range(k // 2, PAIRS - k // 2):
            q = s[j] + t[j] + jnp.where(m, t.get(j + 1, zero), t.get(j - 1, zero))
            if update:
                at = (p - 1) * PAIRS + j
                vx[at_row(p - 1, j), :] = ix[at] * (gx[at] + (qa[PAIRS + j] + q))
            if mid:
                qa[PAIRS + j] = s[j] + jnp.where(m, s.get(j - 1, zero), s.get(j + 1, zero)) + qa[j]
            qa[j] = q

    def sides(k, p):
        return side_sums(arrays_of(k)[1], p, pairs_of(k))

    def keep(k, p, res):
        keep_sums(arrays_of(k)[3], p, res)

    def leave(z):
        return pltpu.make_async_copy(held.at[pl.ds(z, 2)], out.at[pl.ds(z, 2)], out_sem.at[z // 2])

    def unpack(z):
        for u in range(2):
            m = par[u]
            for j in range(HALO // 2, (HALO + Y_DEV) // 2):
                r, b = vr[at_row(HALO + z + u, j), :], vb[at_row(HALO + z + u, j), :]
                y = 2 * j - HALO
                held[z + u, y // 8, pl.ds(y % 8, 8, stride=8), :] = jnp.where(m, r, b)
                held[z + u, y // 8, pl.ds(y % 8 + 1, 8, stride=8), :] = jnp.where(m, b, r)
        leave(z).start()

    for p in range(2):
        keep(1, p, sides(1, p))
    for k in range(1, HALO + 1):
        first = k - 1
        ahead = [sides(k, first + 2 + u) for u in range(2)]
        advance(k, first, first, False, False)
        advance(k, first + 1, first + 1, False, True)
        for u in range(2):
            keep(k, first + 2 + u, ahead[u])
        steps = (EXT - 2 * k) // 2

        def body(p, k=k, first=first, n=2):
            ahead = [sides(k, p + n + u) for u in range(n)]
            for u in range(n):
                advance(k, p + u, first + u, True, True)
            for u in range(n):
                keep(k, p + n + u, ahead[u])

        def body4(i, _, k=k, first=first, body=body):
            p = first + 2 + i * 4
            ahead = [sides(k, p + 2 + u) for u in range(4)]
            advance(k, p, first, True, True)
            advance(k, p + 1, first + 1, True, True)
            for u in range(4):
                keep(k, p + 2 + u, ahead[u])
            advance(k, p + 2, first, True, True)
            advance(k, p + 3, first + 1, True, True)
            if k == HALO:
                unpack(i * 4)
                unpack(i * 4 + 2)
            return 0

        lax.fori_loop(0, (steps - 1) // 2, body4, 0)
        if (steps - 1) % 2:
            body(first + 2 + (steps - 2) * 2)
            if k == HALO:
                unpack((steps - 2) * 2)
        p = first + 2 * steps
        ahead = [sides(k + 1, k + u) for u in range(2)] if k < HALO else []
        advance(k, p, first, True, True)
        advance(k, p + 1, first + 1, True, False)
        for u, res in enumerate(ahead):
            keep(k + 1, k + u, res)
        if k == HALO:
            unpack((steps - 1) * 2)

    for z in range(0, Z_DEV, 2):
        leave(z).wait()


def corner_kernel(odd_ref, zlo, zhi, points, outer, inner):
    odd = odd_ref[0]
    ends = [(Y_DEV // 8 - 1) * side for side in (odd, 1 - odd)]
    starts = [(8 - HALO) * side for side in (odd, 1 - odd)]
    for half, src in enumerate((zlo, zhi)):
        def corner(z, _, half=half, src=src):
            for y in range(HALO):
                at = pl.ds(((half * HALO + z) * HALO + y) * SUB, SUB)
                outer[at, :] = src[z, ends[0], pl.ds(starts[0] + y, 8, stride=8), :]
                inner[at, :] = src[z, ends[1], pl.ds(starts[1] + y, 8, stride=8), :]
            return 0

        lax.fori_loop(0, HALO, corner, 0)
    base = 2 * HALO * HALO * SUB

    def copy(i, _):
        for u in range(8):
            block = points[pl.ds(i * 64 + u * 8, 8), :]
            outer[pl.ds(base + i * 64 + u * 8, 8), :] = block
            inner[pl.ds(base + i * 64 + u * 8, 8), :] = block
        return 0

    lax.fori_loop(0, points.shape[0] // 64, copy, 0)


def as_tiles(a):
    d = a.shape[0]
    a = a.reshape(d, Y_DEV // 8, 8, SUB, LANES).transpose(0, 1, 3, 2, 4)
    return a.reshape(d, Y_DEV // 8, 8 * SUB, LANES)


def shards(slot_brick, slot_count, point_cell, point_frac, point_normal, point_weight, guess):
    n_slab, n_row = lax.axis_size("slab"), lax.axis_size("row")
    peers = point_cell.shape[1]
    tiles = 3 * peers
    slots = tiles * S_PEER

    vmem = pl.BlockSpec(memory_space=pltpu.VMEM)
    smem = pl.BlockSpec(memory_space=pltpu.SMEM)
    hbm = pl.BlockSpec(memory_space=pltpu.HBM)
    small = pltpu.CompilerParams(vmem_limit_bytes=8 * 1024 * 1024)
    split = as_tiles(guess)
    planes = jax.ShapeDtypeStruct((HALO,) + split.shape[1:], F32)
    send, low_planes, high_planes = pl.pallas_call(
        functools.partial(deal_kernel, n_row),
        out_shape=(jax.ShapeDtypeStruct((peers, 3, 8, LANES), F32), planes, planes),
        in_specs=[hbm] * 7,
        out_specs=[vmem] * 3,
        scratch_shapes=[
            pltpu.SMEM((S_PEER, peers), jnp.int32),
            pltpu.SMEM((S_PEER, peers), jnp.int32),
            pltpu.VMEM((peers, S_PEER, CAP), jnp.int32),
            pltpu.VMEM((peers, S_PEER, CAP), F32),
            pltpu.VMEM((peers, 3, S_PEER, CAP), F32),
            pltpu.VMEM((peers, S_PEER, CAP), F32),
            pltpu.SemaphoreType.DMA((8,)),
        ],
        compiler_params=pltpu.CompilerParams(vmem_limit_bytes=60 * 1024 * 1024),
    )(
        slot_brick[0].T, slot_count[0].T, split, point_cell[0], point_frac[0],
        jnp.transpose(point_normal[0], (0, 2, 1, 3)), point_weight[0],
    )

    cells = RIM * RIM
    state = (
        jax.ShapeDtypeStruct((cells, SUB, LANES), F32),
        jax.ShapeDtypeStruct((cells, SUB, LANES), F32),
        jax.ShapeDtypeStruct(((EXT * PAIRS * 9 + 8 + 71) // 72 * 72, LANES), F32),
        jax.ShapeDtypeStruct(((EXT * PAIRS * 9 + 8 + 71) // 72 * 72, LANES), F32),
        jax.ShapeDtypeStruct((EXT * PAIRS, SUB, LANES), F32),
    )
    zlo = lax.ppermute(high_planes, "slab", chain("slab", 1))
    zhi = lax.ppermute(low_planes, "slab", chain("slab", -1))
    got = lax.all_to_all(send, ("slab", "row"), split_axis=0, concat_axis=0, tiled=True)
    ylo = lax.ppermute(split[:, -1], "row", chain("row", 1))
    yhi = lax.ppermute(split[:, 0], "row", chain("row", -1))
    points = got.reshape(tiles * 8, LANES)

    packed = pltpu.VMEM((EXT * PAIRS, SUB, LANES), F32)
    pay = jax.ShapeDtypeStruct((2 * HALO * HALO * SUB + tiles * 8, LANES), F32)
    zi, yi = lax.axis_index("slab"), lax.axis_index("row")
    flags = jnp.stack([zi > 0, zi < n_slab - 1, yi > 0, yi < n_row - 1, yi % 2 == 1]).astype(jnp.int32)
    outer, inner = pl.pallas_call(
        corner_kernel,
        out_shape=(pay, pay),
        in_specs=[smem] + [vmem] * 3,
        out_specs=[vmem] * 2,
        compiler_params=small,
    )(flags[4:], zlo, zhi, points)
    pay_outer = lax.ppermute(outer, "row", swaps("row", 1))
    pay_inner = lax.ppermute(inner, "row", swaps("row", 0))

    def lists(blocks):
        return [
            pltpu.SMEM((blocks * slots + 2 * UNROLL,), jnp.int32),
            pltpu.VMEM((blocks * tiles, LANES), jnp.int32),
            pltpu.SMEM((blocks * tiles, LANES), jnp.int32),
            pltpu.SemaphoreType.DMA((1,)),
        ]

    def limit(blocks, extra):
        return (extra << 20) + 20 * blocks * slots * LANES * 4

    held = pl.pallas_call(
        functools.partial(near_kernel, tiles),
        out_shape=state,
        in_specs=[vmem] * 6,
        out_specs=[vmem] * 5,
        scratch_shapes=[
            pltpu.VMEM((20, slots + 8, LANES), F32),
            pltpu.VMEM((4 * UNROLL, SUB, LANES), F32),
        ] + lists(1),
        cost_estimate=pl.CostEstimate(flops=40_000_000_000, bytes_accessed=1_000_000, transcendentals=0),
        compiler_params=pltpu.CompilerParams(vmem_limit_bytes=limit(1, 6)),
    )(split, zlo, zhi, ylo, yhi, points)
    out = pl.pallas_call(
        functools.partial(relax_kernel, tiles),
        out_shape=state + (jax.ShapeDtypeStruct((Z_DEV, Y_DEV // 8, 8 * SUB, LANES), F32),),
        in_specs=[smem] + [vmem] * 7,
        out_specs=[vmem] * 5 + [hbm],
        input_output_aliases={3 + i: i for i in range(5)},
        scratch_shapes=[
            pltpu.VMEM((20, 2 * slots + 8, LANES), F32),
            pltpu.VMEM((4 * UNROLL, SUB, LANES), F32),
            packed, packed, packed, packed, packed,
            pltpu.VMEM((2 * PAIRS, SUB, LANES), F32),
            pltpu.VMEM((Z_DEV, Y_DEV // 8, 8 * SUB, LANES), F32),
            pltpu.SemaphoreType.DMA((Z_DEV // 2,)),
        ] + lists(2),
        compiler_params=pltpu.CompilerParams(vmem_limit_bytes=limit(2, 18)),
    )(flags, pay_outer, pay_inner, *held)[-1]
    out = out.reshape(Z_DEV, Y_DEV // 8, SUB, 8, LANES).transpose(0, 1, 3, 2, 4)
    return out.reshape(Z_DEV, Y_DEV, NX)


def solution(mesh):
    placed = (
        P(("slab", "row"), None, None),
        P(("slab", "row"), None, None),
        P(("slab", "row"), None, None, None),
        P(("slab", "row"), None, None, None),
        P(("slab", "row"), None, None, None, None),
        P(("slab", "row"), None, None, None),
        P("slab", "row", None),
    )
    return jax.shard_map(
        shards, mesh=mesh, in_specs=placed, out_specs=P("slab", "row", None), check_vma=False
    )
```

```python
import functools
import jax
import jax.numpy as jnp
from jax import lax
from jax.experimental import pallas as pl
from jax.experimental.pallas import tpu as pltpu
from jax.sharding import PartitionSpec as P

Z_DEV = 16
Y_DEV = 16
NX = 1024
CAP = 64
S_PEER = 2
SWEEPS = 3
ALPHA = 4.0

HALO = 2 * SWEEPS
EXT = Z_DEV + 2 * HALO
PAIRS = EXT // 2
RIM = EXT + 2
LANES = 128
SUB = NX // LANES
CODE = 16384
UNROLL = 16
F32 = jnp.float32
BF16 = jnp.bfloat16


def chain(axis, step):
    size = lax.axis_size(axis)
    return [(i, i + step) for i in range(size) if 0 <= i + step < size]


def swaps(axis, start):
    pairs = [(i, i + 1) for i in range(start, lax.axis_size(axis) - 1, 2)]
    return pairs + [(j, i) for i, j in pairs]


def lane_sets():
    lane = lax.broadcasted_iota(jnp.int32, (SUB, LANES), 1)
    even = lane % 2 == 0
    return lane < CAP, (even, jnp.logical_not(even)), lane == 0, lane == LANES - 1


def brick_rows(pay, tiles):
    peers = tiles // 3
    parts = max(1, S_PEER * peers // LANES)
    found = []
    for which in range(3):
        for part in range(parts):
            total = jnp.zeros((8, LANES), F32)
            for i in range(peers // 8):
                total = total + pay[pl.ds(i * 192 + which * 8 + 6 + part, 8, stride=24), :]
            found.append(jnp.sum(total, axis=0, keepdims=True))
    found.append(jnp.zeros((8 - len(found), LANES), F32))
    return jnp.concatenate(found, axis=0)


def find_places(bricks, tiles, block, dy, entries):
    parts = max(1, S_PEER * tiles // 3 // LANES)
    lane = lax.broadcasted_iota(jnp.int32, (8, LANES), 1)
    sub = lax.broadcasted_iota(jnp.int32, (8, LANES), 0)
    brick = bricks.astype(jnp.int32) - 1
    if parts == 1:
        which, at = sub, lane
    else:
        which, at = sub >> 1, ((sub & 1) << 7) + lane
    t = (at >> 1) * 3 + which
    z = (brick >> 4) + HALO + Z_DEV * (which - 1)
    y = (brick & (Y_DEV - 1)) + HALO + Y_DEV * dy
    inside = (brick >= 0) & (z >= 0) & (z < EXT) & (y >= 0) & (y < EXT)
    row = block * tiles * S_PEER + (((t >> 3) * 2 + (at & 1)) << 3) + (t & 7)
    entries[pl.ds(block * 8, 8), :] = jnp.where(inside, ((z + 1) * RIM + y + 1) * CODE + row, -1)


def prepare_points(pays, tiles, step, prep, places, todo):
    low = lane_sets()[0]
    slots = tiles * S_PEER
    width = min(LANES, S_PEER * tiles // 3)
    group = width // (8 * S_PEER)
    dummy = (RIM + 1) * CODE + len(pays) * slots
    for u in range(UNROLL):
        todo[u] = jnp.int32(dummy)
    pos = jnp.int32(UNROLL)
    for block, (pay, base) in enumerate(pays):
        def prepare(i, pos, pay=pay, base=base, block=block):
            work = []
            for g in range(group):
                for s in range(S_PEER):
                    at = base + (i * group + g) * (8 * step) + s
                    rows = [pay[pl.ds(at + 2 * r, 8, stride=step), :] for r in range(3)]
                    work.append((g, s, rows, [pltpu.roll(x, CAP, 1) for x in rows]))
            for c in range(0, width, 8):
                found = [places[block * 8 + i, c + k] for k in range(8)]
                for e in found:
                    todo[pos] = e
                    pos = pos + (1 + (e >> 31))
            for g, s, rows, turned in work:
                cell = jnp.where(low, rows[0], turned[0])
                frac = jnp.where(low, turned[0], rows[0])
                vals = []
                for r in (1, 2):
                    vals.append(jnp.where(low, rows[r], turned[r]))
                    vals.append(jnp.where(low, turned[r], rows[r]))
                less = 0.5 - frac
                more = 0.5 + frac
                weights = (
                    jnp.where(low, 0.5 * less * less, 0.75 - frac * frac),
                    jnp.where(low, 0.5 * more * more, 0.0),
                )
                whole = cell.astype(jnp.int32)
                at = pl.multiple_of(block * slots + ((i * group + g) * 2 + s) * 8, 8)
                for h in range(2):
                    c = jnp.where(low, whole - 1, whole) if h == 0 else whole + 1
                    prep[16 + h, pl.ds(at, 8), :] = (c >> 7).astype(F32)
                    prep[18 + h, pl.ds(at, 8), :] = (c & 127).astype(F32)
                    for ch in range(4):
                        v = vals[ch] * weights[h]
                        head = v.astype(BF16).astype(F32)
                        prep[h * 8 + ch, pl.ds(at, 8), :] = head
                        prep[h * 8 + 4 + ch, pl.ds(at, 8), :] = v - head
            return pos

        pos = lax.fori_loop(0, tiles // (8 * group), prepare, pos)
    zero = jnp.zeros((SUB, LANES), F32)
    for q in range(20):
        prep[q, pl.ds(len(pays) * slots, 8), :] = zero
    for u in range(UNROLL):
        todo[pos + u] = jnp.int32(dummy)
    return pos - UNROLL


def splat_slots(count, todo, prep, stage, accd, accr):
    sub = lax.broadcasted_iota(jnp.int32, (SUB, LANES), 0)
    subf = sub.astype(F32)
    keep_up = (sub > 0).astype(F32)
    keep_dn = (sub < SUB - 1).astype(F32)
    first_lane, last_lane = lane_sets()[2:]
    col = lax.broadcasted_iota(jnp.int32, (LANES, LANES), 0).astype(F32).astype(BF16)
    one = jnp.ones((LANES, LANES), BF16)
    nil = jnp.zeros((LANES, LANES), BF16)
    for q in range(4 * UNROLL):
        stage[q] = jnp.zeros((SUB, LANES), F32)

    def add(i):
        slopes = []
        for u in range(UNROLL):
            v = stage[4 * u]
            up = jnp.where(last_lane, pltpu.roll(v, 1, 0) * keep_up, v)
            dn = jnp.where(first_lane, pltpu.roll(v, SUB - 1, 0) * keep_dn, v)
            slopes.append(pltpu.roll(dn, LANES - 1, 1) - pltpu.roll(up, 1, 1))
        for u in range(UNROLL):
            centre = todo[i * UNROLL + u] >> 14
            f1, f2, f3 = (stage[4 * u + ch] for ch in range(1, 4))
            new = [
                accd[centre] + f3,
                accr[centre] + slopes[u],
                accr[centre + 1] + f1,
                accr[centre - 1] - f1,
                accr[centre + RIM] + f2,
                accr[centre - RIM] - f2,
            ]
            accd[centre] = new[0]
            accr[centre] = new[1]
            accr[centre + 1] = new[2]
            accr[centre - 1] = new[3]
            accr[centre + RIM] = new[4]
            accr[centre - RIM] = new[5]

    def splat(i, _):
        add(i)
        sums = []
        for u in range(UNROLL):
            row = todo[(i + 1) * UNROLL + u] & (CODE - 1)
            lhs, rhs = [], []
            for h in range(2):
                hi = jnp.broadcast_to(prep[16 + h, pl.ds(row, 1), :], (SUB, LANES))
                hit = hi == subf
                parts = [
                    jnp.where(hit, jnp.broadcast_to(prep[h * 8 + q, pl.ds(row, 1), :], (SUB, LANES)), 0.0)
                    for q in range(8)
                ]
                lhs.append(jnp.concatenate(parts, axis=0))
                lo = jnp.broadcast_to(prep[18 + h, pl.ds(row, 1), :], (LANES, LANES)).astype(BF16)
                rhs.append(jnp.where(lo == col, one, nil))
            left = jnp.concatenate(lhs, axis=1).astype(BF16)
            right = jnp.concatenate(rhs, axis=1)
            res = lax.dot_general(left, right, (((1,), (1,)), ((), ())), preferred_element_type=F32)
            sums.append([res[ch * 8:ch * 8 + 8] + res[32 + ch * 8:40 + ch * 8] for ch in range(4)])
        for u in range(UNROLL):
            for ch in range(4):
                stage[4 * u + ch] = sums[u][ch]
        return 0

    groups = (count + UNROLL - 1) // UNROLL
    lax.fori_loop(0, groups, splat, 0)
    add(groups)


def at_row(z, j):
    return pl.ds((z * PAIRS + j) * 9 + 1, SUB)


def pack_pair(vr, vb, z, j, m, a, b):
    vr[at_row(z, j), :] = jnp.where(m, a, b)
    vb[at_row(z, j), :] = jnp.where(m, b, a)


def side_sums(v, z, pairs):
    first_lane, last_lane = lane_sets()[2:]
    res = []
    for j in pairs:
        at = (z * PAIRS + j) * 9
        x = v[pl.ds(at + 1, SUB), :]
        up = jnp.where(last_lane, v[pl.ds(at, SUB), :], x)
        dn = jnp.where(first_lane, v[pl.ds(at + 2, SUB), :], x)
        res.append((j, pltpu.roll(up, 1, 1) + pltpu.roll(dn, LANES - 1, 1)))
    return res


def keep_sums(sums, z, res):
    for j, value in res:
        sums[z * PAIRS + j] = value


def slab_kernel(guess, outer, inner, held, sem_in, sem_out):
    odd = lax.axis_index("slab") % 2
    far = Z_DEV - HALO
    half = HALO // 2
    into, out = [], []
    for i, (first, dst) in enumerate(((far * odd, outer), (far * (1 - odd), inner))):
        for k in range(2):
            n = i * 2 + k
            into.append(pltpu.make_async_copy(guess.at[pl.ds(first + k * half, half)], held.at[n], sem_in.at[n]))
            out.append(pltpu.make_async_copy(held.at[n], dst.at[pl.ds(k * half, half)], sem_out.at[n]))
    for move in into:
        move.start()
    for first, second in zip(into, out):
        first.wait()
        second.start()
    for move in out:
        move.wait()


def deal_kernel(n_row, brick_in, number_in, cell_in, frac_in, normal_in, weight_in, send,
                brick, number, cell, frac, normal, weight, sem):
    loads = [
        pltpu.make_async_copy(src, dst, sem.at[i])
        for i, (src, dst) in enumerate((
            (brick_in, brick), (number_in, number), (cell_in, cell), (frac_in, frac), (normal_in, normal),
            (weight_in, weight),
        ))
    ]
    for load in loads:
        load.start()
    peers = cell.shape[0]
    lane = lax.broadcasted_iota(jnp.int32, (S_PEER, CAP), 1)
    sub = lax.broadcasted_iota(jnp.int32, (S_PEER, CAP), 0)
    mine = (lax.axis_index("slab") * n_row + lax.axis_index("row")) * S_PEER
    wide = lax.broadcasted_iota(jnp.int32, (2, LANES), 1) + LANES * lax.broadcasted_iota(jnp.int32, (2, LANES), 0)
    empty = jnp.zeros((8, LANES), F32)
    for d in range(n_row):
        send[d, 0] = empty
        send[peers - 1 - d, 2] = empty
    group = 4
    for load in loads:
        load.wait()

    def tile(i, _):
        for g in range(group):
            d = i * group + g
            live = (lane < jnp.where(sub == 0, number[0, d], number[1, d])).astype(F32)
            place = jnp.where(wide == mine, brick[0, d] + 1, jnp.where(wide == mine + 1, brick[1, d] + 1, 0))
            pieces = (
                jnp.concatenate([cell[d].astype(F32), frac[d]], axis=1),
                jnp.concatenate([normal[d, 0] * (-3.0 * live), normal[d, 1] * (3.0 * live)], axis=1),
                jnp.concatenate([normal[d, 2] * (3.0 * live), weight[d] * live], axis=1),
                place.astype(F32),
            )
            for r, piece in enumerate(pieces):
                send[d, 1, 2 * r:2 * r + 2, :] = piece
        return 0

    lax.fori_loop(0, peers // group, tile, 0)

    def spread(i, _):
        for g in range(group):
            d = i * group + g
            block = send[d, 1]
            below = send[d + n_row, 1]
            send[d + n_row, 0] = block
            send[d, 2] = below
        return 0

    lax.fori_loop(0, (peers - n_row) // group, spread, 0)


def near_kernel(tiles, guess, z_outer, z_inner, ylo, yhi, points, accd, accr, vr, vb, sr,
                prep, stage, todo, entries, places, sem):
    zero = jnp.zeros((SUB, LANES), F32)
    par = lane_sets()[1]
    odd_slab = lax.axis_index("slab") % 2
    high = HALO + Z_DEV
    find_places(brick_rows(points, tiles), tiles, 0, 0, entries)
    fetch = pltpu.make_async_copy(entries, places, sem.at[0])
    fetch.start()

    def clear(i, _):
        for u in range(12):
            accd[i * 12 + u] = zero
            accr[i * 12 + u] = zero
        return 0

    lax.fori_loop(0, RIM * RIM // 12, clear, 0)

    def clear_v(i, _):
        for u in range(9):
            vr[pl.ds(i * 72 + u * 8, 8), :] = zero
            vb[pl.ds(i * 72 + u * 8, 8), :] = zero
        return 0

    lax.fori_loop(0, vr.shape[0] // 72, clear_v, 0)

    def edges(i, _):
        for u in range(2):
            for src, z0 in ((z_outer, high * odd_slab), (z_inner, high * (1 - odd_slab))):
                zi = i * 2 + u
                for j in range(Y_DEV // 2):
                    a = src[zi, 2 * j // 8, pl.ds(2 * j % 8, 8, stride=8), :]
                    b = src[zi, 2 * j // 8, pl.ds(2 * j % 8 + 1, 8, stride=8), :]
                    pack_pair(vr, vb, z0 + zi, HALO // 2 + j, par[u], a, b)
        return 0

    def middle(i, _):
        for u in range(2):
            zi = i * 2 + u
            for j in range(Y_DEV // 2):
                a = guess[zi, 2 * j // 8, pl.ds(2 * j % 8, 8, stride=8), :]
                b = guess[zi, 2 * j // 8, pl.ds(2 * j % 8 + 1, 8, stride=8), :]
                pack_pair(vr, vb, HALO + zi, HALO // 2 + j, par[u], a, b)
            for j in range(HALO // 2):
                y = 8 - HALO + 2 * j
                a, b = (ylo[zi, pl.ds(y + k, 8, stride=8), :] for k in range(2))
                pack_pair(vr, vb, HALO + zi, j, par[u], a, b)
                a, b = (yhi[zi, pl.ds(2 * j + k, 8, stride=8), :] for k in range(2))
                pack_pair(vr, vb, HALO + zi, (HALO + Y_DEV) // 2 + j, par[u], a, b)
        return 0

    lax.fori_loop(0, HALO // 2, edges, 0)
    lax.fori_loop(0, Z_DEV // 2, middle, 0)

    def first_sums(i, _):
        res = [side_sums(vr, i * 4 + u, range(PAIRS)) for u in range(4)]
        for u in range(4):
            keep_sums(sr, i * 4 + u, res[u])
        return 0

    lax.fori_loop(0, EXT // 4, first_sums, 0)
    fetch.wait()
    count = prepare_points(((points, 0),), tiles, 8, prep, places, todo)
    splat_slots(count, todo, prep, stage, accd, accr)


def relax_kernel(tiles, flags, pay_outer, pay_inner, *refs):
    accd, accr, vr, vb, sr, out = refs[5:11]
    prep, stage, gr, gb, ir, ib, sb, qa, held, out_sem, todo, entries, places, sem = refs[11:]
    par = lane_sets()[1]
    zero = jnp.zeros((SUB, LANES), F32)
    base = 2 * HALO * HALO * SUB
    pays = ((pay_outer, base), (pay_inner, base))
    at_zlo, at_zhi, at_ylo, at_yhi, odd = (flags[k] for k in range(5))
    side = 2 * odd - 1
    last = pl.ds(base + tiles * 6, 8)
    find_places(pay_outer[last, :], tiles, 0, side, entries)
    find_places(pay_inner[last, :], tiles, 1, -side, entries)
    high = (HALO + Y_DEV) // 2
    fetch = pltpu.make_async_copy(entries, places, sem.at[0])
    fetch.start()

    edge_pairs = (*range(HALO // 2), *range((HALO + Y_DEV) // 2, PAIRS))

    def corners(i, _):
        for half in range(2):
            for u in range(2):
                zi = half * HALO + i * 2 + u
                z = zi + half * Z_DEV
                for j in range(HALO // 2):
                    for pay, j0 in ((pay_outer, high * odd), (pay_inner, high * (1 - odd))):
                        a, b = (pay[pl.ds((zi * HALO + 2 * j + k) * SUB, SUB), :] for k in range(2))
                        pack_pair(vr, vb, z, j0 + j, par[u], a, b)
        for half in range(2):
            for u in range(2):
                z = half * (HALO + Z_DEV) + i * 2 + u
                keep_sums(sr, z, side_sums(vr, z, edge_pairs))
        return 0

    lax.fori_loop(0, HALO // 2, corners, 0)
    fetch.wait()
    count = prepare_points(pays, tiles, 6, prep, places, todo)
    splat_slots(count, todo, prep, stage, accd, accr)

    def finish(i, _):
        for u in range(2):
            z = 1 + i * 2 + u
            m = par[(1 + u) % 2]
            fz = jnp.where(z < HALO, at_zlo, jnp.where(z >= HALO + Z_DEV, at_zhi, 1))
            for j in range(PAIRS):
                fy = at_ylo if j < HALO // 2 else at_yhi if j >= (HALO + Y_DEV) // 2 else None
                f = fz if fy is None else fz * fy
                scale = jnp.broadcast_to(f.astype(F32) * (1.0 / 6.0), (SUB, LANES))
                r = (z + 1) * RIM + 2 * j + 1
                da, db = accd[r], accd[r + 1]
                ra, rb = accr[r], accr[r + 1]
                at = z * PAIRS + j
                ir[at] = scale / (8.0 / 3.0 + ALPHA * jnp.where(m, da, db))
                ib[at] = scale / (8.0 / 3.0 + ALPHA * jnp.where(m, db, da))
                gr[at] = jnp.where(m, ra, rb)
                gb[at] = jnp.where(m, rb, ra)
        return 0

    lax.fori_loop(0, (EXT - 2) // 2, finish, 0)

    def pairs_of(k):
        return [j for j in range(k // 2 - 1, PAIRS + 1 - k // 2) if 0 <= j < PAIRS]

    def arrays_of(k):
        return (vr, vb, sr, sb, gr, ir) if k % 2 else (vb, vr, sb, sr, gb, ib)

    def advance(k, p, pp, update, mid):
        vx, _, sums, others, gx, ix = arrays_of(k)
        m = par[((k - 1) % 2 + pp) % 2]
        s, t = {}, {}
        for j in pairs_of(k):
            s[j] = sums[p * PAIRS + j]
            t[j] = vx[at_row(p, j), :] + 0.5 * others[p * PAIRS + j]
        for j in range(k // 2, PAIRS - k // 2):
            q = s[j] + t[j] + jnp.where(m, t.get(j + 1, zero), t.get(j - 1, zero))
            if update:
                at = (p - 1) * PAIRS + j
                vx[at_row(p - 1, j), :] = ix[at] * (gx[at] + (qa[PAIRS + j] + q))
            if mid:
                qa[PAIRS + j] = s[j] + jnp.where(m, s.get(j - 1, zero), s.get(j + 1, zero)) + qa[j]
            qa[j] = q

    def sides(k, p):
        return side_sums(arrays_of(k)[1], p, pairs_of(k))

    def keep(k, p, res):
        keep_sums(arrays_of(k)[3], p, res)

    def leave(z):
        return pltpu.make_async_copy(held.at[pl.ds(z, 2)], out.at[pl.ds(z, 2)], out_sem.at[z // 2])

    def unpack(z):
        for u in range(2):
            m = par[u]
            for j in range(HALO // 2, (HALO + Y_DEV) // 2):
                r, b = vr[at_row(HALO + z + u, j), :], vb[at_row(HALO + z + u, j), :]
                y = 2 * j - HALO
                held[z + u, y // 8, pl.ds(y % 8, 8, stride=8), :] = jnp.where(m, r, b)
                held[z + u, y // 8, pl.ds(y % 8 + 1, 8, stride=8), :] = jnp.where(m, b, r)
        leave(z).start()

    for p in range(2):
        keep(1, p, sides(1, p))
    for k in range(1, HALO + 1):
        first = k - 1
        ahead = [sides(k, first + 2 + u) for u in range(2)]
        advance(k, first, first, False, False)
        advance(k, first + 1, first + 1, False, True)
        for u in range(2):
            keep(k, first + 2 + u, ahead[u])
        steps = (EXT - 2 * k) // 2

        def body(p, k=k, first=first, n=2):
            ahead = [sides(k, p + n + u) for u in range(n)]
            for u in range(n):
                advance(k, p + u, first + u, True, True)
            for u in range(n):
                keep(k, p + n + u, ahead[u])

        def body4(i, _, k=k, first=first, body=body):
            p = first + 2 + i * 4
            ahead = [sides(k, p + 2 + u) for u in range(4)]
            advance(k, p, first, True, True)
            advance(k, p + 1, first + 1, True, True)
            for u in range(4):
                keep(k, p + 2 + u, ahead[u])
            advance(k, p + 2, first, True, True)
            advance(k, p + 3, first + 1, True, True)
            if k == HALO:
                unpack(i * 4)
                unpack(i * 4 + 2)
            return 0

        lax.fori_loop(0, (steps - 1) // 2, body4, 0)
        if (steps - 1) % 2:
            body(first + 2 + (steps - 2) * 2)
            if k == HALO:
                unpack((steps - 2) * 2)
        p = first + 2 * steps
        ahead = [sides(k + 1, k + u) for u in range(2)] if k < HALO else []
        advance(k, p, first, True, True)
        advance(k, p + 1, first + 1, True, False)
        for u, res in enumerate(ahead):
            keep(k + 1, k + u, res)
        if k == HALO:
            unpack((steps - 1) * 2)

    for z in range(0, Z_DEV, 2):
        leave(z).wait()


def corner_kernel(z_outer, z_inner, points, outer, inner):
    odd = lax.axis_index("row") % 2
    odd_slab = lax.axis_index("slab") % 2
    ends = [(Y_DEV // 8 - 1) * side for side in (odd, 1 - odd)]
    starts = [(8 - HALO) * side for side in (odd, 1 - odd)]
    for half, src in ((odd_slab, z_outer), (1 - odd_slab, z_inner)):
        def corner(z, _, half=half, src=src):
            for y in range(HALO):
                at = pl.ds(((half * HALO + z) * HALO + y) * SUB, SUB)
                outer[at, :] = src[z, ends[0], pl.ds(starts[0] + y, 8, stride=8), :]
                inner[at, :] = src[z, ends[1], pl.ds(starts[1] + y, 8, stride=8), :]
            return 0

        lax.fori_loop(0, HALO, corner, 0)
    base = 2 * HALO * HALO * SUB
    tiles = points.shape[0] // 8

    def copy(i, _):
        for u in range(8):
            block = points[pl.ds((i * 8 + u) * 8, 8), :]
            at = pl.ds(base + (i * 8 + u) * 6, 8)
            outer[at, :] = block
            inner[at, :] = block
        return 0

    lax.fori_loop(0, tiles // 8, copy, 0)
    bricks = brick_rows(points, tiles)
    outer[pl.ds(base + tiles * 6, 8), :] = bricks
    inner[pl.ds(base + tiles * 6, 8), :] = bricks


def as_tiles(a):
    d = a.shape[0]
    a = a.reshape(d, Y_DEV // 8, 8, SUB, LANES).transpose(0, 1, 3, 2, 4)
    return a.reshape(d, Y_DEV // 8, 8 * SUB, LANES)


def shards(slot_brick, slot_count, point_cell, point_frac, point_normal, point_weight, guess):
    n_slab, n_row = lax.axis_size("slab"), lax.axis_size("row")
    peers = point_cell.shape[1]
    tiles = 3 * peers
    slots = tiles * S_PEER

    vmem = pl.BlockSpec(memory_space=pltpu.VMEM)
    smem = pl.BlockSpec(memory_space=pltpu.SMEM)
    hbm = pl.BlockSpec(memory_space=pltpu.HBM)
    small = pltpu.CompilerParams(vmem_limit_bytes=8 * 1024 * 1024)
    split = as_tiles(guess)
    planes = jax.ShapeDtypeStruct((HALO,) + split.shape[1:], F32)
    outer, inner = pl.pallas_call(
        slab_kernel,
        out_shape=(planes, planes),
        in_specs=[hbm],
        out_specs=[hbm] * 2,
        scratch_shapes=[
            pltpu.VMEM((4, HALO // 2) + split.shape[1:], F32),
            pltpu.SemaphoreType.DMA((4,)),
            pltpu.SemaphoreType.DMA((4,)),
        ],
        compiler_params=small,
    )(pltpu.with_memory_space_constraint(split, pltpu.HBM))

    cells = RIM * RIM
    state = (
        jax.ShapeDtypeStruct((cells, SUB, LANES), F32),
        jax.ShapeDtypeStruct((cells, SUB, LANES), F32),
        jax.ShapeDtypeStruct(((EXT * PAIRS * 9 + 8 + 71) // 72 * 72, LANES), F32),
        jax.ShapeDtypeStruct(((EXT * PAIRS * 9 + 8 + 71) // 72 * 72, LANES), F32),
        jax.ShapeDtypeStruct((EXT * PAIRS, SUB, LANES), F32),
    )
    z_outer = lax.ppermute(outer, "slab", swaps("slab", 1))
    z_inner = lax.ppermute(inner, "slab", swaps("slab", 0))
    send = pl.pallas_call(
        functools.partial(deal_kernel, n_row),
        out_shape=jax.ShapeDtypeStruct((peers, 3, 8, LANES), F32),
        in_specs=[hbm] * 6,
        out_specs=vmem,
        scratch_shapes=[
            pltpu.SMEM((S_PEER, peers), jnp.int32),
            pltpu.SMEM((S_PEER, peers), jnp.int32),
            pltpu.VMEM((peers, S_PEER, CAP), jnp.int32),
            pltpu.VMEM((peers, S_PEER, CAP), F32),
            pltpu.VMEM((peers, 3, S_PEER, CAP), F32),
            pltpu.VMEM((peers, S_PEER, CAP), F32),
            pltpu.SemaphoreType.DMA((6,)),
        ],
        compiler_params=small,
    )(*(pltpu.with_memory_space_constraint(a, pltpu.HBM) for a in (
        slot_brick[0].T, slot_count[0].T, point_cell[0], point_frac[0],
        jnp.transpose(point_normal[0], (0, 2, 1, 3)), point_weight[0],
    )))
    got = lax.all_to_all(send, ("slab", "row"), split_axis=0, concat_axis=0, tiled=True)
    ylo = lax.ppermute(split[:, -1], "row", chain("row", 1))
    yhi = lax.ppermute(split[:, 0], "row", chain("row", -1))
    points = got.reshape(tiles * 8, LANES)

    packed = pltpu.VMEM((EXT * PAIRS, SUB, LANES), F32)
    pay = jax.ShapeDtypeStruct((2 * HALO * HALO * SUB + tiles * 6 + 8, LANES), F32)
    zi, yi = lax.axis_index("slab"), lax.axis_index("row")
    flags = jnp.stack([zi > 0, zi < n_slab - 1, yi > 0, yi < n_row - 1, yi % 2 == 1]).astype(jnp.int32)
    row_outer, row_inner = pl.pallas_call(
        corner_kernel,
        out_shape=(pay, pay),
        in_specs=[vmem] * 3,
        out_specs=[vmem] * 2,
        compiler_params=small,
    )(z_outer, z_inner, points)
    pay_outer = lax.ppermute(row_outer, "row", swaps("row", 1))
    pay_inner = lax.ppermute(row_inner, "row", swaps("row", 0))

    def lists(blocks):
        return [
            pltpu.SMEM((blocks * slots + 2 * UNROLL,), jnp.int32),
            pltpu.VMEM((blocks * 8, LANES), jnp.int32),
            pltpu.SMEM((blocks * 8, LANES), jnp.int32),
            pltpu.SemaphoreType.DMA((1,)),
        ]

    def limit(blocks, extra):
        return (extra << 20) + 20 * blocks * slots * LANES * 4

    held = pl.pallas_call(
        functools.partial(near_kernel, tiles),
        out_shape=state,
        in_specs=[vmem] * 6,
        out_specs=[vmem] * 5,
        scratch_shapes=[
            pltpu.VMEM((20, slots + 8, LANES), F32),
            pltpu.VMEM((4 * UNROLL, SUB, LANES), F32),
        ] + lists(1),
        cost_estimate=pl.CostEstimate(flops=40_000_000_000, bytes_accessed=1_000_000, transcendentals=0),
        compiler_params=pltpu.CompilerParams(vmem_limit_bytes=limit(1, 6)),
    )(split, z_outer, z_inner, ylo, yhi, points)
    out = pl.pallas_call(
        functools.partial(relax_kernel, tiles),
        out_shape=state + (jax.ShapeDtypeStruct((Z_DEV, Y_DEV // 8, 8 * SUB, LANES), F32),),
        in_specs=[smem] + [vmem] * 7,
        out_specs=[vmem] * 5 + [hbm],
        input_output_aliases={3 + i: i for i in range(5)},
        scratch_shapes=[
            pltpu.VMEM((20, 2 * slots + 8, LANES), F32),
            pltpu.VMEM((4 * UNROLL, SUB, LANES), F32),
            packed, packed, packed, packed, packed,
            pltpu.VMEM((2 * PAIRS, SUB, LANES), F32),
            pltpu.VMEM((Z_DEV, Y_DEV // 8, 8 * SUB, LANES), F32),
            pltpu.SemaphoreType.DMA((Z_DEV // 2,)),
        ] + lists(2),
        compiler_params=pltpu.CompilerParams(vmem_limit_bytes=limit(2, 18)),
    )(flags, pay_outer, pay_inner, *held)[-1]
    out = out.reshape(Z_DEV, Y_DEV // 8, SUB, 8, LANES).transpose(0, 1, 3, 2, 4)
    return out.reshape(Z_DEV, Y_DEV, NX)


def solution(mesh):
    placed = (
        P(("slab", "row"), None, None),
        P(("slab", "row"), None, None),
        P(("slab", "row"), None, None, None),
        P(("slab", "row"), None, None, None),
        P(("slab", "row"), None, None, None, None),
        P(("slab", "row"), None, None, None),
        P("slab", "row", None),
    )
    return jax.shard_map(
        shards, mesh=mesh, in_specs=placed, out_specs=P("slab", "row", None), check_vma=False
    )
```

```python
import functools
import jax
import jax.numpy as jnp
from jax import lax
from jax.experimental import pallas as pl
from jax.experimental.pallas import tpu as pltpu
from jax.sharding import PartitionSpec as P

Z_DEV = 16
Y_DEV = 16
NX = 1024
CAP = 64
S_PEER = 2
SWEEPS = 3
ALPHA = 4.0

HALO = 2 * SWEEPS
EXT = Z_DEV + 2 * HALO
PAIRS = EXT // 2
RIM = EXT + 2
LANES = 128
SUB = NX // LANES
CODE = 16384
UNROLL = 16
STRIDE = 12
F32 = jnp.float32
BF16 = jnp.bfloat16


def chain(axis, step):
    size = lax.axis_size(axis)
    return [(i, i + step) for i in range(size) if 0 <= i + step < size]


def swaps(axis, start):
    pairs = [(i, i + 1) for i in range(start, lax.axis_size(axis) - 1, 2)]
    return pairs + [(j, i) for i, j in pairs]


def lane_sets():
    lane = lax.broadcasted_iota(jnp.int32, (SUB, LANES), 1)
    even = lane % 2 == 0
    return lane < CAP, (even, jnp.logical_not(even)), lane == 0, lane == LANES - 1


def brick_rows(pay, tiles):
    peers = tiles // 3
    parts = max(1, S_PEER * peers // LANES)
    found = []
    for which in range(3):
        for part in range(parts):
            total = jnp.zeros((8, LANES), F32)
            for i in range(peers // 8):
                total = total + pay[pl.ds(i * 192 + which * 8 + 6 + part, 8, stride=24), :]
            found.append(jnp.sum(total, axis=0, keepdims=True))
    found.append(jnp.zeros((8 - len(found), LANES), F32))
    return jnp.concatenate(found, axis=0)


def find_places(bricks, tiles, block, dy, entries):
    parts = max(1, S_PEER * tiles // 3 // LANES)
    lane = lax.broadcasted_iota(jnp.int32, (8, LANES), 1)
    sub = lax.broadcasted_iota(jnp.int32, (8, LANES), 0)
    brick = bricks.astype(jnp.int32) - 1
    if parts == 1:
        which, at = sub, lane
    else:
        which, at = sub >> 1, ((sub & 1) << 7) + lane
    t = (at >> 1) * 3 + which
    z = (brick >> 4) + HALO + Z_DEV * (which - 1)
    y = (brick & (Y_DEV - 1)) + HALO + Y_DEV * dy
    inside = (brick >= 0) & (z >= 0) & (z < EXT) & (y >= 0) & (y < EXT)
    row = block * tiles * S_PEER + (((t >> 3) * 2 + (at & 1)) << 3) + (t & 7)
    entries[pl.ds(block * 8, 8), :] = jnp.where(inside, ((z + 1) * RIM + y + 1) * CODE + row, -1)


def prepare_points(pays, tiles, step, prep, places, todo):
    low = lane_sets()[0]
    slots = tiles * S_PEER
    width = min(LANES, S_PEER * tiles // 3)
    group = width // (8 * S_PEER)
    dummy = (RIM + 1) * CODE + len(pays) * slots
    for u in range(UNROLL):
        todo[u] = jnp.int32(dummy)
    pos = jnp.int32(UNROLL)
    for block, (pay, base) in enumerate(pays):
        def prepare(i, pos, pay=pay, base=base, block=block):
            work = []
            for g in range(group):
                for s in range(S_PEER):
                    at = base + (i * group + g) * (8 * step) + s
                    rows = [pay[pl.ds(at + 2 * r, 8, stride=step), :] for r in range(3)]
                    work.append((g, s, rows, [pltpu.roll(x, CAP, 1) for x in rows]))
            for c in range(0, width, 8):
                found = [places[block * 8 + i, c + k] for k in range(8)]
                for e in found:
                    todo[pos] = e
                    pos = pos + (1 + (e >> 31))
            for g, s, rows, turned in work:
                cell = jnp.where(low, rows[0], turned[0])
                frac = jnp.where(low, turned[0], rows[0])
                vals = []
                for r in (1, 2):
                    vals.append(jnp.where(low, rows[r], turned[r]))
                    vals.append(jnp.where(low, turned[r], rows[r]))
                less = 0.5 - frac
                more = 0.5 + frac
                weights = (
                    jnp.where(low, 0.5 * less * less, 0.75 - frac * frac),
                    jnp.where(low, 0.5 * more * more, 0.0),
                )
                whole = cell.astype(jnp.int32)
                at = pl.multiple_of(block * slots + ((i * group + g) * 2 + s) * 8, 8)
                for h in range(2):
                    c = jnp.where(low, whole - 1, whole) if h == 0 else whole + 1
                    prep[16 + h, pl.ds(at, 8), :] = (c >> 7).astype(F32)
                    prep[18 + h, pl.ds(at, 8), :] = (c & 127).astype(F32)
                    for ch in range(4):
                        v = vals[ch] * weights[h]
                        head = v.astype(BF16).astype(F32)
                        prep[h * 8 + ch, pl.ds(at, 8), :] = head
                        prep[h * 8 + 4 + ch, pl.ds(at, 8), :] = v - head
            return pos

        pos = lax.fori_loop(0, tiles // (8 * group), prepare, pos)
    zero = jnp.zeros((SUB, LANES), F32)
    for q in range(20):
        prep[q, pl.ds(len(pays) * slots, 8), :] = zero
    for u in range(UNROLL):
        todo[pos + u] = jnp.int32(dummy)
    return pos - UNROLL


def splat_slots(count, todo, prep, stage, accd, accr):
    sub = lax.broadcasted_iota(jnp.int32, (SUB, LANES), 0)
    subf = sub.astype(F32)
    keep_up = (sub > 0).astype(F32)
    keep_dn = (sub < SUB - 1).astype(F32)
    first_lane, last_lane = lane_sets()[2:]
    col = lax.broadcasted_iota(jnp.int32, (LANES, LANES), 0).astype(F32).astype(BF16)
    one = jnp.ones((LANES, LANES), BF16)
    nil = jnp.zeros((LANES, LANES), BF16)
    for q in range(4 * UNROLL):
        stage[q] = jnp.zeros((SUB, LANES), F32)

    def add(i):
        slopes = []
        for u in range(UNROLL):
            v = stage[4 * u]
            up = jnp.where(last_lane, pltpu.roll(v, 1, 0) * keep_up, v)
            dn = jnp.where(first_lane, pltpu.roll(v, SUB - 1, 0) * keep_dn, v)
            slopes.append(pltpu.roll(dn, LANES - 1, 1) - pltpu.roll(up, 1, 1))
        for u in range(UNROLL):
            centre = todo[i * UNROLL + u] >> 14
            f1, f2, f3 = (stage[4 * u + ch] for ch in range(1, 4))
            new = [
                accd[centre] + f3,
                accr[centre] + slopes[u],
                accr[centre + 1] + f1,
                accr[centre - 1] - f1,
                accr[centre + RIM] + f2,
                accr[centre - RIM] - f2,
            ]
            accd[centre] = new[0]
            accr[centre] = new[1]
            accr[centre + 1] = new[2]
            accr[centre - 1] = new[3]
            accr[centre + RIM] = new[4]
            accr[centre - RIM] = new[5]

    def splat(i, _):
        add(i)
        sums = []
        for u in range(UNROLL):
            row = todo[(i + 1) * UNROLL + u] & (CODE - 1)
            lhs, rhs = [], []
            for h in range(2):
                hi = jnp.broadcast_to(prep[16 + h, pl.ds(row, 1), :], (SUB, LANES))
                hit = hi == subf
                parts = [
                    jnp.where(hit, jnp.broadcast_to(prep[h * 8 + q, pl.ds(row, 1), :], (SUB, LANES)), 0.0)
                    for q in range(8)
                ]
                lhs.append(jnp.concatenate(parts, axis=0))
                lo = jnp.broadcast_to(prep[18 + h, pl.ds(row, 1), :], (LANES, LANES)).astype(BF16)
                rhs.append(jnp.where(lo == col, one, nil))
            left = jnp.concatenate(lhs, axis=1).astype(BF16)
            right = jnp.concatenate(rhs, axis=1)
            res = lax.dot_general(left, right, (((1,), (1,)), ((), ())), preferred_element_type=F32)
            sums.append([res[ch * 8:ch * 8 + 8] + res[32 + ch * 8:40 + ch * 8] for ch in range(4)])
        for u in range(UNROLL):
            for ch in range(4):
                stage[4 * u + ch] = sums[u][ch]
        return 0

    groups = (count + UNROLL - 1) // UNROLL
    lax.fori_loop(0, groups, splat, 0)
    add(groups)


def at_row(z, j):
    return pl.ds((z * PAIRS + j) * 9 + 1, SUB)


def pack_pair(vr, vb, z, j, m, a, b):
    vr[at_row(z, j), :] = jnp.where(m, a, b)
    vb[at_row(z, j), :] = jnp.where(m, b, a)


def side_sums(v, z, pairs):
    first_lane, last_lane = lane_sets()[2:]
    res = []
    for j in pairs:
        at = (z * PAIRS + j) * 9
        x = v[pl.ds(at + 1, SUB), :]
        up = jnp.where(last_lane, v[pl.ds(at, SUB), :], x)
        dn = jnp.where(first_lane, v[pl.ds(at + 2, SUB), :], x)
        res.append((j, pltpu.roll(up, 1, 1) + pltpu.roll(dn, LANES - 1, 1)))
    return res


def keep_sums(sums, z, res):
    for j, value in res:
        sums[z * PAIRS + j] = value


def slab_kernel(guess, outer, inner, held, sem_in, sem_out):
    odd = lax.axis_index("slab") % 2
    far = Z_DEV - HALO
    half = HALO // 2
    into, out = [], []
    for i, (first, dst) in enumerate(((far * odd, outer), (far * (1 - odd), inner))):
        for k in range(2):
            n = i * 2 + k
            into.append(pltpu.make_async_copy(guess.at[pl.ds(first + k * half, half)], held.at[n], sem_in.at[n]))
            out.append(pltpu.make_async_copy(held.at[n], dst.at[pl.ds(k * half, half)], sem_out.at[n]))
    for move in into:
        move.start()
    for first, second in zip(into, out):
        first.wait()
        second.start()
    for move in out:
        move.wait()


def deal_kernel(n_row, brick_in, number_in, cell_in, frac_in, normal_in, weight_in, send,
                brick, number, cell, frac, normal, weight, sem):
    loads = [
        pltpu.make_async_copy(src, dst, sem.at[i])
        for i, (src, dst) in enumerate((
            (brick_in, brick), (number_in, number), (cell_in, cell), (frac_in, frac), (normal_in, normal),
            (weight_in, weight),
        ))
    ]
    for load in loads:
        load.start()
    peers = cell.shape[0]
    lane = lax.broadcasted_iota(jnp.int32, (S_PEER, CAP), 1)
    sub = lax.broadcasted_iota(jnp.int32, (S_PEER, CAP), 0)
    mine = (lax.axis_index("slab") * n_row + lax.axis_index("row")) * S_PEER
    wide = lax.broadcasted_iota(jnp.int32, (2, LANES), 1) + LANES * lax.broadcasted_iota(jnp.int32, (2, LANES), 0)
    empty = jnp.zeros((8, LANES), F32)
    for d in range(n_row):
        send[d, 0] = empty
        send[peers - 1 - d, 2] = empty
    group = 4
    for load in loads:
        load.wait()

    def tile(i, _):
        for g in range(group):
            d = i * group + g
            live = (lane < jnp.where(sub == 0, number[0, d], number[1, d])).astype(F32)
            place = jnp.where(wide == mine, brick[0, d] + 1, jnp.where(wide == mine + 1, brick[1, d] + 1, 0))
            pieces = (
                jnp.concatenate([cell[d].astype(F32), frac[d]], axis=1),
                jnp.concatenate([normal[d, 0] * (-3.0 * live), normal[d, 1] * (3.0 * live)], axis=1),
                jnp.concatenate([normal[d, 2] * (3.0 * live), weight[d] * live], axis=1),
                place.astype(F32),
            )
            for r, piece in enumerate(pieces):
                send[d, 1, 2 * r:2 * r + 2, :] = piece
        return 0

    lax.fori_loop(0, peers // group, tile, 0)

    def spread(i, _):
        for g in range(group):
            d = i * group + g
            block = send[d, 1]
            below = send[d + n_row, 1]
            send[d + n_row, 0] = block
            send[d, 2] = below
        return 0

    lax.fori_loop(0, (peers - n_row) // group, spread, 0)


def near_kernel(tiles, guess, z_outer, z_inner, ylo, yhi, points, accd, accr, vr, vb, sr,
                prep, stage, todo, entries, places, sem):
    zero = jnp.zeros((SUB, LANES), F32)
    par = lane_sets()[1]
    odd_slab = lax.axis_index("slab") % 2
    high = HALO + Z_DEV
    find_places(brick_rows(points, tiles), tiles, 0, 0, entries)
    fetch = pltpu.make_async_copy(entries, places, sem.at[0])
    fetch.start()

    def clear(i, _):
        for u in range(12):
            accd[i * 12 + u] = zero
            accr[i * 12 + u] = zero
        return 0

    lax.fori_loop(0, RIM * RIM // 12, clear, 0)

    def clear_v(i, _):
        for u in range(9):
            vr[pl.ds(i * 72 + u * 8, 8), :] = zero
            vb[pl.ds(i * 72 + u * 8, 8), :] = zero
        return 0

    lax.fori_loop(0, vr.shape[0] // 72, clear_v, 0)

    def edges(i, _):
        for u in range(2):
            for src, z0 in ((z_outer, high * odd_slab), (z_inner, high * (1 - odd_slab))):
                zi = i * 2 + u
                for j in range(Y_DEV // 2):
                    a = src[zi, 2 * j // 8, pl.ds(2 * j % 8, 8, stride=8), :]
                    b = src[zi, 2 * j // 8, pl.ds(2 * j % 8 + 1, 8, stride=8), :]
                    pack_pair(vr, vb, z0 + zi, HALO // 2 + j, par[u], a, b)
        return 0

    def middle(i, _):
        for u in range(2):
            zi = i * 2 + u
            for j in range(Y_DEV // 2):
                a = guess[zi, 2 * j // 8, pl.ds(2 * j % 8, 8, stride=8), :]
                b = guess[zi, 2 * j // 8, pl.ds(2 * j % 8 + 1, 8, stride=8), :]
                pack_pair(vr, vb, HALO + zi, HALO // 2 + j, par[u], a, b)
            for j in range(HALO // 2):
                y = 8 - HALO + 2 * j
                a, b = (ylo[zi, pl.ds(y + k, 8, stride=8), :] for k in range(2))
                pack_pair(vr, vb, HALO + zi, j, par[u], a, b)
                a, b = (yhi[zi, pl.ds(2 * j + k, 8, stride=8), :] for k in range(2))
                pack_pair(vr, vb, HALO + zi, (HALO + Y_DEV) // 2 + j, par[u], a, b)
        return 0

    lax.fori_loop(0, HALO // 2, edges, 0)
    lax.fori_loop(0, Z_DEV // 2, middle, 0)

    def first_sums(i, _):
        res = [side_sums(vr, i * 4 + u, range(PAIRS)) for u in range(4)]
        for u in range(4):
            keep_sums(sr, i * 4 + u, res[u])
        return 0

    lax.fori_loop(0, EXT // 4, first_sums, 0)
    fetch.wait()
    count = prepare_points(((points, 0),), tiles, 8, prep, places, todo)
    splat_slots(count, todo, prep, stage, accd, accr)


def relax_kernel(tiles, flags, pay_outer, pay_inner, *refs):
    accd, accr, vr, vb, sr, out = refs[5:11]
    prep, stage, gr, gb, ir, ib, sb, qa, held, out_sem, todo, entries, places, sem = refs[11:]
    par = lane_sets()[1]
    zero = jnp.zeros((SUB, LANES), F32)
    base = 2 * HALO * HALO * SUB
    pays = ((pay_outer, base), (pay_inner, base))
    at_zlo, at_zhi, at_ylo, at_yhi, odd = (flags[k] for k in range(5))
    side = 2 * odd - 1
    last = pl.ds(base + tiles * 6, 8)
    find_places(pay_outer[last, :], tiles, 0, side, entries)
    find_places(pay_inner[last, :], tiles, 1, -side, entries)
    high = (HALO + Y_DEV) // 2
    fetch = pltpu.make_async_copy(entries, places, sem.at[0])
    fetch.start()

    edge_pairs = (*range(HALO // 2), *range((HALO + Y_DEV) // 2, PAIRS))

    def corners(i, _):
        for half in range(2):
            for u in range(2):
                zi = half * HALO + i * 2 + u
                z = zi + half * Z_DEV
                for j in range(HALO // 2):
                    for pay, j0 in ((pay_outer, high * odd), (pay_inner, high * (1 - odd))):
                        a, b = (pay[pl.ds((zi * HALO + 2 * j + k) * SUB, SUB), :] for k in range(2))
                        pack_pair(vr, vb, z, j0 + j, par[u], a, b)
        for half in range(2):
            for u in range(2):
                z = half * (HALO + Z_DEV) + i * 2 + u
                keep_sums(sr, z, side_sums(vr, z, edge_pairs))
        return 0

    lax.fori_loop(0, HALO // 2, corners, 0)
    fetch.wait()
    count = prepare_points(pays, tiles, 6, prep, places, todo)
    splat_slots(count, todo, prep, stage, accd, accr)

    def finish(i, _):
        for u in range(2):
            z = 1 + i * 2 + u
            m = par[(1 + u) % 2]
            fz = jnp.where(z < HALO, at_zlo, jnp.where(z >= HALO + Z_DEV, at_zhi, 1))
            for j in range(PAIRS):
                fy = at_ylo if j < HALO // 2 else at_yhi if j >= (HALO + Y_DEV) // 2 else None
                f = fz if fy is None else fz * fy
                scale = jnp.broadcast_to(f.astype(F32) * (1.0 / 6.0), (SUB, LANES))
                r = (z + 1) * RIM + 2 * j + 1
                da, db = accd[r], accd[r + 1]
                ra, rb = accr[r], accr[r + 1]
                at = z * PAIRS + j
                ir[at] = scale / (8.0 / 3.0 + ALPHA * jnp.where(m, da, db))
                ib[at] = scale / (8.0 / 3.0 + ALPHA * jnp.where(m, db, da))
                gr[at] = jnp.where(m, ra, rb)
                gb[at] = jnp.where(m, rb, ra)
        return 0

    lax.fori_loop(0, (EXT - 2) // 2, finish, 0)

    def pairs_of(k):
        return [j for j in range(k // 2 - 1, PAIRS + 1 - k // 2) if 0 <= j < PAIRS]

    def arrays_of(k):
        return (vr, vb, sr, sb, gr, ir) if k % 2 else (vb, vr, sb, sr, gb, ib)

    def advance(k, p, pp, update, mid):
        vx, _, sums, others, gx, ix = arrays_of(k)
        m = par[((k - 1) % 2 + pp) % 2]
        s, t = {}, {}
        for j in pairs_of(k):
            s[j] = sums[p * PAIRS + j]
            t[j] = vx[at_row(p, j), :] + 0.5 * others[p * PAIRS + j]
        for j in range(k // 2, PAIRS - k // 2):
            q = s[j] + t[j] + jnp.where(m, t.get(j + 1, zero), t.get(j - 1, zero))
            if update:
                at = (p - 1) * PAIRS + j
                vx[at_row(p - 1, j), :] = ix[at] * (gx[at] + (qa[PAIRS + j] + q))
            if mid:
                qa[PAIRS + j] = s[j] + jnp.where(m, s.get(j - 1, zero), s.get(j + 1, zero)) + qa[j]
            qa[j] = q

    def sides(k, p):
        return side_sums(arrays_of(k)[1], p, pairs_of(k))

    def keep(k, p, res):
        keep_sums(arrays_of(k)[3], p, res)

    def leave(z):
        return pltpu.make_async_copy(held.at[pl.ds(z, 2)], out.at[pl.ds(z, 2)], out_sem.at[z // 2])

    def unpack(z):
        for u in range(2):
            m = par[u]
            for j in range(HALO // 2, (HALO + Y_DEV) // 2):
                r, b = vr[at_row(HALO + z + u, j), :], vb[at_row(HALO + z + u, j), :]
                y = 2 * j - HALO
                held[z + u, y // 8, pl.ds(y % 8, 8, stride=8), :] = jnp.where(m, r, b)
                held[z + u, y // 8, pl.ds(y % 8 + 1, 8, stride=8), :] = jnp.where(m, b, r)
        leave(z).start()

    for p in range(2):
        keep(1, p, sides(1, p))
    for k in range(1, HALO + 1):
        first = k - 1
        ahead = [sides(k, first + 2 + u) for u in range(2)]
        advance(k, first, first, False, False)
        advance(k, first + 1, first + 1, False, True)
        for u in range(2):
            keep(k, first + 2 + u, ahead[u])
        steps = (EXT - 2 * k) // 2

        def body(p, count, k=k, first=first):
            for c in range(0, 2 * count, 2):
                ahead = [sides(k, p + c + 2 + u) for u in range(2)]
                advance(k, p + c, first, True, True)
                advance(k, p + c + 1, first + 1, True, True)
                for u in range(2):
                    keep(k, p + c + 2 + u, ahead[u])
                if k == HALO:
                    unpack(p + c - first - 2)

        loops, rest = divmod(steps - 1, STRIDE)
        if rest:
            body(first + 2, rest)

        def run(i, _, k=k, start=first + 2 + 2 * rest, body=body):
            body(start + i * (2 * STRIDE), STRIDE)
            return 0

        if loops:
            lax.fori_loop(0, loops, run, 0)
        p = first + 2 * steps
        ahead = [sides(k + 1, k + u) for u in range(2)] if k < HALO else []
        advance(k, p, first, True, True)
        advance(k, p + 1, first + 1, True, False)
        for u, res in enumerate(ahead):
            keep(k + 1, k + u, res)
        if k == HALO:
            unpack((steps - 1) * 2)

    for z in range(0, Z_DEV, 2):
        leave(z).wait()


def corner_kernel(z_outer, z_inner, points, outer, inner):
    odd = lax.axis_index("row") % 2
    odd_slab = lax.axis_index("slab") % 2
    ends = [(Y_DEV // 8 - 1) * side for side in (odd, 1 - odd)]
    starts = [(8 - HALO) * side for side in (odd, 1 - odd)]
    for half, src in ((odd_slab, z_outer), (1 - odd_slab, z_inner)):
        def corner(z, _, half=half, src=src):
            for y in range(HALO):
                at = pl.ds(((half * HALO + z) * HALO + y) * SUB, SUB)
                outer[at, :] = src[z, ends[0], pl.ds(starts[0] + y, 8, stride=8), :]
                inner[at, :] = src[z, ends[1], pl.ds(starts[1] + y, 8, stride=8), :]
            return 0

        lax.fori_loop(0, HALO, corner, 0)
    base = 2 * HALO * HALO * SUB
    tiles = points.shape[0] // 8

    def copy(i, _):
        for u in range(8):
            block = points[pl.ds((i * 8 + u) * 8, 8), :]
            at = pl.ds(base + (i * 8 + u) * 6, 8)
            outer[at, :] = block
            inner[at, :] = block
        return 0

    lax.fori_loop(0, tiles // 8, copy, 0)
    bricks = brick_rows(points, tiles)
    outer[pl.ds(base + tiles * 6, 8), :] = bricks
    inner[pl.ds(base + tiles * 6, 8), :] = bricks


def as_tiles(a):
    d = a.shape[0]
    a = a.reshape(d, Y_DEV // 8, 8, SUB, LANES).transpose(0, 1, 3, 2, 4)
    return a.reshape(d, Y_DEV // 8, 8 * SUB, LANES)


def shards(slot_brick, slot_count, point_cell, point_frac, point_normal, point_weight, guess):
    n_slab, n_row = lax.axis_size("slab"), lax.axis_size("row")
    peers = point_cell.shape[1]
    tiles = 3 * peers
    slots = tiles * S_PEER

    vmem = pl.BlockSpec(memory_space=pltpu.VMEM)
    smem = pl.BlockSpec(memory_space=pltpu.SMEM)
    hbm = pl.BlockSpec(memory_space=pltpu.HBM)
    small = pltpu.CompilerParams(vmem_limit_bytes=8 * 1024 * 1024)
    split = as_tiles(guess)
    planes = jax.ShapeDtypeStruct((HALO,) + split.shape[1:], F32)
    outer, inner = pl.pallas_call(
        slab_kernel,
        out_shape=(planes, planes),
        in_specs=[hbm],
        out_specs=[hbm] * 2,
        scratch_shapes=[
            pltpu.VMEM((4, HALO // 2) + split.shape[1:], F32),
            pltpu.SemaphoreType.DMA((4,)),
            pltpu.SemaphoreType.DMA((4,)),
        ],
        compiler_params=small,
    )(pltpu.with_memory_space_constraint(split, pltpu.HBM))

    cells = RIM * RIM
    state = (
        jax.ShapeDtypeStruct((cells, SUB, LANES), F32),
        jax.ShapeDtypeStruct((cells, SUB, LANES), F32),
        jax.ShapeDtypeStruct(((EXT * PAIRS * 9 + 8 + 71) // 72 * 72, LANES), F32),
        jax.ShapeDtypeStruct(((EXT * PAIRS * 9 + 8 + 71) // 72 * 72, LANES), F32),
        jax.ShapeDtypeStruct((EXT * PAIRS, SUB, LANES), F32),
    )
    z_outer = lax.ppermute(outer, "slab", swaps("slab", 1))
    z_inner = lax.ppermute(inner, "slab", swaps("slab", 0))
    send = pl.pallas_call(
        functools.partial(deal_kernel, n_row),
        out_shape=jax.ShapeDtypeStruct((peers, 3, 8, LANES), F32),
        in_specs=[hbm] * 6,
        out_specs=vmem,
        scratch_shapes=[
            pltpu.SMEM((S_PEER, peers), jnp.int32),
            pltpu.SMEM((S_PEER, peers), jnp.int32),
            pltpu.VMEM((peers, S_PEER, CAP), jnp.int32),
            pltpu.VMEM((peers, S_PEER, CAP), F32),
            pltpu.VMEM((peers, 3, S_PEER, CAP), F32),
            pltpu.VMEM((peers, S_PEER, CAP), F32),
            pltpu.SemaphoreType.DMA((6,)),
        ],
        compiler_params=small,
    )(*(pltpu.with_memory_space_constraint(a, pltpu.HBM) for a in (
        slot_brick[0].T, slot_count[0].T, point_cell[0], point_frac[0],
        jnp.transpose(point_normal[0], (0, 2, 1, 3)), point_weight[0],
    )))
    got = lax.all_to_all(send, ("slab", "row"), split_axis=0, concat_axis=0, tiled=True)
    ylo = lax.ppermute(split[:, -1], "row", chain("row", 1))
    yhi = lax.ppermute(split[:, 0], "row", chain("row", -1))
    points = got.reshape(tiles * 8, LANES)

    packed = pltpu.VMEM((EXT * PAIRS, SUB, LANES), F32)
    pay = jax.ShapeDtypeStruct((2 * HALO * HALO * SUB + tiles * 6 + 8, LANES), F32)
    zi, yi = lax.axis_index("slab"), lax.axis_index("row")
    flags = jnp.stack([zi > 0, zi < n_slab - 1, yi > 0, yi < n_row - 1, yi % 2 == 1]).astype(jnp.int32)
    row_outer, row_inner = pl.pallas_call(
        corner_kernel,
        out_shape=(pay, pay),
        in_specs=[vmem] * 3,
        out_specs=[vmem] * 2,
        compiler_params=small,
    )(z_outer, z_inner, points)
    pay_outer = lax.ppermute(row_outer, "row", swaps("row", 1))
    pay_inner = lax.ppermute(row_inner, "row", swaps("row", 0))

    def lists(blocks):
        return [
            pltpu.SMEM((blocks * slots + 2 * UNROLL,), jnp.int32),
            pltpu.VMEM((blocks * 8, LANES), jnp.int32),
            pltpu.SMEM((blocks * 8, LANES), jnp.int32),
            pltpu.SemaphoreType.DMA((1,)),
        ]

    def limit(blocks, extra):
        return (extra << 20) + 20 * blocks * slots * LANES * 4

    held = pl.pallas_call(
        functools.partial(near_kernel, tiles),
        out_shape=state,
        in_specs=[vmem] * 6,
        out_specs=[vmem] * 5,
        scratch_shapes=[
            pltpu.VMEM((20, slots + 8, LANES), F32),
            pltpu.VMEM((4 * UNROLL, SUB, LANES), F32),
        ] + lists(1),
        cost_estimate=pl.CostEstimate(flops=40_000_000_000, bytes_accessed=1_000_000, transcendentals=0),
        compiler_params=pltpu.CompilerParams(vmem_limit_bytes=limit(1, 6)),
    )(split, z_outer, z_inner, ylo, yhi, points)
    out = pl.pallas_call(
        functools.partial(relax_kernel, tiles),
        out_shape=state + (jax.ShapeDtypeStruct((Z_DEV, Y_DEV // 8, 8 * SUB, LANES), F32),),
        in_specs=[smem] + [vmem] * 7,
        out_specs=[vmem] * 5 + [hbm],
        input_output_aliases={3 + i: i for i in range(5)},
        scratch_shapes=[
            pltpu.VMEM((20, 2 * slots + 8, LANES), F32),
            pltpu.VMEM((4 * UNROLL, SUB, LANES), F32),
            packed, packed, packed, packed, packed,
            pltpu.VMEM((2 * PAIRS, SUB, LANES), F32),
            pltpu.VMEM((Z_DEV, Y_DEV // 8, 8 * SUB, LANES), F32),
            pltpu.SemaphoreType.DMA((Z_DEV // 2,)),
        ] + lists(2),
        compiler_params=pltpu.CompilerParams(vmem_limit_bytes=limit(2, 18)),
    )(flags, pay_outer, pay_inner, *held)[-1]
    out = out.reshape(Z_DEV, Y_DEV // 8, SUB, 8, LANES).transpose(0, 1, 3, 2, 4)
    return out.reshape(Z_DEV, Y_DEV, NX)


def solution(mesh):
    placed = (
        P(("slab", "row"), None, None),
        P(("slab", "row"), None, None),
        P(("slab", "row"), None, None, None),
        P(("slab", "row"), None, None, None),
        P(("slab", "row"), None, None, None, None),
        P(("slab", "row"), None, None, None),
        P("slab", "row", None),
    )
    return jax.shard_map(
        shards, mesh=mesh, in_specs=placed, out_specs=P("slab", "row", None), check_vma=False
    )
```
